256 devices in a mesh: ga: 32 (over y, x, z_hi), band: 8 (over z_lo, core).
Axes of the slice: x: 4, y: 4, z: 8 (z_hi: 2, z_lo: 4; z = z_hi * 4 + z_lo), core: 2. Of those that a mesh axis runs over, the one named last changes fastest.
Arguments:
- coefficients: float32 [2048, 2, 16384], P('band', None, 'ga'), may hold values from -6 to 6
- rotation: float32 [2, 2048, 256], P(None, 'band', 'ga'), may hold values from -0.1875 to 0.1875
- potential: float32 [64, 4096], P(None, 'ga'), may hold values from -2 to 0.5
- index_map: int32 [16384], replicated, may hold values from 0 to 262143, as said below
- counts: int32 [32], replicated, may hold values from 384 to 512, as said below
Outputs:
- applied_panel: float32 [256, 2, 32, 1024], P(('band', 'ga'))
The draws below stay inside these ranges and needn't reach their ends.
Inputs may be any that keep to these rules, and one draw needn't show every extreme that they name: counts[i] counts the live slots of index i of ga, which are its slots 0 to counts[i] - 1 of 512; the counts sum to 14336, and some index has exactly 512. `index_map`: live slots name distinct cells, and together exactly 14336 cells whose signed frequency vector has a squared length no larger than that of any cell not named (a ball about the anchor), every signed component of a live cell lying in -16 to 15; dead slots name arbitrary cells.
All inputs are finite; a program needn't handle non-finite values.
Results may differ from the reference program's by a relative error of at most 0.00008.
Values sent between devices are 32-bit elements; how exact they have to be, the bound alone decides.
A program may use at most 128 MiB of HBM per device.

```python
import jax
import jax.numpy as jnp
from jax import lax

BANDS = 2048
BOX = 64
SLOT_DEV = 512
PW_DEV = 448
NPW = 14336
PANEL = 256
N_GA = 32


def layout_draw(key):
    folded = jax.random.fold_in(key, 7)
    key_ties, key_shuffle, key_pairs, key_order, key_dead = jax.random.split(folded, 5)
    cell_count = BOX * BOX * BOX
    flat_cells = jnp.arange(cell_count, dtype=jnp.int32)
    freq_x = flat_cells // (BOX * BOX)
    freq_y = flat_cells // BOX % BOX
    freq_z = flat_cells % BOX
    freq_x = jnp.where(freq_x >= BOX // 2, freq_x - BOX, freq_x)
    freq_y = jnp.where(freq_y >= BOX // 2, freq_y - BOX, freq_y)
    freq_z = jnp.where(freq_z >= BOX // 2, freq_z - BOX, freq_z)
    squared_norm = freq_x * freq_x + freq_y * freq_y + freq_z * freq_z
    ties_rank = jax.random.permutation(key_ties, cell_count).astype(jnp.int32)
    ranking = jnp.argsort(squared_norm * cell_count + ties_rank, stable=True).astype(jnp.int32)
    ball_cells = jax.random.permutation(key_shuffle, ranking[:NPW])
    dead_mean = SLOT_DEV - PW_DEV
    pair_count = N_GA // 2
    shifts = jax.random.randint(key_pairs, (pair_count,), -dead_mean, dead_mean + 1).astype(jnp.int32)
    shifts = shifts.at[0].set(dead_mean)
    dead_slots = jnp.concatenate([dead_mean + shifts, dead_mean - shifts])
    dead_slots = jax.random.permutation(key_order, dead_slots)
    counts = (SLOT_DEV - dead_slots).astype(jnp.int32)
    offsets = jnp.cumsum(counts) - counts
    slot_ids = jnp.arange(SLOT_DEV, dtype=jnp.int32)
    slot_pos = jnp.clip(offsets[:, None] + slot_ids[None, :], 0, NPW - 1)
    live_mask = slot_ids[None, :] < counts[:, None]
    filler = jax.random.randint(key_dead, (N_GA, SLOT_DEV), 0, cell_count).astype(jnp.int32)
    index_map = jnp.where(live_mask, ball_cells[slot_pos], filler).reshape(-1).astype(jnp.int32)
    return (index_map, counts)


def draw_index_map(key, part):
    return layout_draw(key)[0]


def draw_counts(key, part):
    return layout_draw(key)[1]


def spiked(entries, rng, source, target, shards_of, factor):
    owner, partner = [(jnp.arange(entries.shape[dim]) // (entries.shape[dim] // shards_of)).reshape([-1 if axis == dim else 1 for axis in range(entries.ndim)]) for dim in (source, target)]
    chosen = jax.random.permutation(rng, shards_of)[partner]
    strong = (owner == chosen) | (owner == (partner + shards_of // 2) % shards_of)
    return jnp.where(strong, factor * entries, entries)


def level_of(own_key, extent, cuts, least, largest):
    level = 1.0
    for axis_at, shards_of in cuts:
        draws = jax.random.uniform(jax.random.fold_in(jax.random.fold_in(own_key, 6), axis_at), (shards_of,), jnp.float32, least / len(cuts), largest / len(cuts))
        level = level * jnp.repeat(jnp.exp(draws), extent[axis_at] // shards_of).reshape((-1,) + (1,) * (len(extent) - 1 - axis_at))
    return level


def normal_values(rng, extent, deviation, limit, pieces=(), held_as=jnp.bfloat16):
    values = deviation * jax.random.normal(rng, extent, jnp.float32)
    if pieces:
        values = values * level_of(rng, extent, pieces, -0.22, 0.18)
    return jnp.clip(values, -limit, limit).astype(held_as)


def noise_with(key, dims, width, limit, pieces, heavy, kind=jnp.bfloat16):
    result = width * jax.random.normal(key, dims, jnp.float32)
    if pieces:
        result = result * level_of(key, dims, pieces, -0.22, 0.18)
    return jnp.clip(spiked(result, jax.random.fold_in(key, 3), *heavy), -limit, limit).astype(kind)


def setup_inputs(seed: int = 0) -> dict:
    streams_of = jax.random.split(jax.random.key(seed), 6)
    coefficients = normal_values(streams_of[0], (BANDS, 2, SLOT_DEV * N_GA), 1.0, 6.0, ((0, 8), (2, 32)), jnp.float32)
    rotation = noise_with(streams_of[1], (2, BANDS, PANEL), (2 * BANDS) ** -0.5, 0.1875, ((1, 8), (2, 32)), (1, 2, 32, 2.75), jnp.float32)
    potential = jnp.clip(-2.0 + 2.5 * jax.random.uniform(streams_of[2], (BOX, BOX * BOX), jnp.float32) ** level_of(streams_of[2], (BOX, BOX * BOX), ((1, 32),), -0.2, 0.2), -2.0, 0.5)
    index_map = draw_index_map(jax.random.fold_in(streams_of[5], 71), 0)
    counts = draw_counts(jax.random.fold_in(streams_of[5], 71), 0)
    return {"coefficients": coefficients, "rotation": rotation, "potential": potential, "index_map": index_map, "counts": counts}


def mixing(columns):
    real_cols = columns[0].T
    imag_cols = columns[1].T
    upper_rows = jnp.stack([real_cols, -imag_cols], axis=-1)
    lower_rows = jnp.stack([imag_cols, real_cols], axis=-1)
    stacked = jnp.stack([upper_rows, lower_rows], axis=1)
    return stacked.reshape(2 * real_cols.shape[0], 2 * real_cols.shape[1])


def kinetic_grid(box_edge):
    ticks_index = jnp.arange(box_edge, dtype=jnp.int32)
    signed = jnp.where(ticks_index >= box_edge // 2, ticks_index - box_edge, ticks_index).astype(jnp.float32)
    squared = signed[:, None, None] ** 2 + signed[None, :, None] ** 2 + signed[None, None, :] ** 2
    return (8.0 / (box_edge * box_edge)) * squared


def reference(coefficients, rotation, potential, index_map, counts):
    band_count = coefficients.shape[0]
    slot_total = coefficients.shape[2]
    mixer_rows = mixing(rotation)
    rotated = jnp.dot(mixer_rows, coefficients.reshape(2 * band_count, slot_total),
                      precision=lax.Precision.HIGHEST).reshape(PANEL, 2, slot_total)
    slot_ids = jnp.arange(SLOT_DEV, dtype=jnp.int32)
    live_mask = (slot_ids[None, :] < counts[:, None]).reshape(-1).astype(jnp.float32)
    kinetic = kinetic_grid(BOX)
    pot_grid = potential.reshape(BOX, BOX, BOX)
    window = BOX // 2
    window_ids = ((jnp.arange(window, dtype=jnp.int32) - window // 2) % BOX).astype(jnp.int32)

    def one_band(values):
        masked = values * live_mask[None, :]
        box_cells = jnp.zeros((2, BOX * BOX * BOX), jnp.float32).at[:, index_map].add(masked)
        grid_field = (box_cells[0] + 1j * box_cells[1]).reshape(BOX, BOX, BOX)
        real_space = jnp.fft.ifftn(grid_field)
        applied = jnp.fft.fftn(pot_grid * real_space) + kinetic * grid_field
        applied = jnp.take(applied, window_ids, axis=0)
        applied = jnp.take(applied, window_ids, axis=1)
        applied = jnp.take(applied, window_ids, axis=2)
        return jnp.stack([applied.real, applied.imag]).reshape(2, window, window * window)

    return lax.map(one_band, rotated)
```

```python
import math
import numpy as np
import jax
import jax.numpy as jnp
from jax import lax
from jax.experimental import pallas as pl
from jax.experimental.pallas import tpu as pltpu

F32 = jnp.float32
BF = jnp.bfloat16
HS = 72
FS = 40


def split_np(a):
    a = np.asarray(a, np.float32)
    hi = a.astype(BF)
    lo = (a - hi.astype(np.float32)).astype(BF)
    return hi, lo


def stack3(a):
    hi, lo = split_np(a)
    return np.concatenate([hi, hi, lo], axis=1)


def tables():
    n = np.arange(32) - 16
    r = np.arange(64)
    ang = 2.0 * math.pi * ((r[:, None] * n[None, :]) % 64) / 64.0
    cos, sin = np.cos(ang), np.sin(ang)
    perm = np.array([(k % 8) * 4 + k // 8 for k in range(32)])
    s = 8.0 / 4096.0
    wz = np.zeros((2, 4, 32, 2, 4, 2, 64))
    for q in range(4):
        wz[0, q, :, 0, q, 0, :] = cos.T / 64
        wz[1, q, :, 0, q, 0, :] = -sin.T / 64
        wz[0, q, :, 0, q, 1, :] = sin.T / 64
        wz[1, q, :, 0, q, 1, :] = cos.T / 64
    wz[:, :, :, 1] = wz[:, :, :, 0] * (s * n * n)[None, None, :, None, None, None]
    wz_h, wz_l = split_np(wz.reshape(256, 1024))
    ty = stack3(np.concatenate([cos[:, perm], sin[:, perm]], axis=1) / 64)
    tx = stack3(np.concatenate([cos, sin], axis=1) / 64)
    fx = stack3(np.concatenate([cos.T, sin.T], axis=0))
    fy = stack3(np.concatenate([cos.T[perm], sin.T[perm]], axis=0))
    wf = np.zeros((4, 2, 64, 2, 4, 32))
    for q in range(4):
        wf[q, 0, :, 0, q, :] = cos
        wf[q, 1, :, 0, q, :] = sin
        wf[q, 1, :, 1, q, :] = cos
        wf[q, 0, :, 1, q, :] = -sin
    wf_h, wf_l = split_np(wf.reshape(512, 256))
    return [wz_h, wz_l, ty, tx, fx, fy, wf_h, wf_l]


def split(a):
    hi = a.astype(BF)
    return hi, (a - hi.astype(F32)).astype(BF)


def dot(a, b):
    return jnp.dot(a, b, preferred_element_type=F32)


def apply_kernel(
    counts, vals, idx, pot, wz_h, wz_l, ty, tx, fx, fy, wf_h, wf_l, out,
    acc, ek, h, f, g, o,
):
    lane = lax.broadcasted_iota(jnp.int32, (1, 128), 1)
    turn = jnp.where(lane < 64, -1.0, 1.0).astype(F32)
    rows128 = lax.broadcasted_iota(jnp.int32, (128, 512), 0)
    rows256 = lax.broadcasted_iota(jnp.int32, (256, 512), 0)
    slot = lax.broadcasted_iota(jnp.int32, (1, 512), 1)

    acc[...] = jnp.zeros_like(acc)

    def place(i, _):
        cols, rows = [], []
        for q in range(4):
            k = i * 4 + q
            cell = idx[pl.ds(k, 1), :]
            wx = ((cell >> 12) + 16) & 63
            wy = ((cell >> 6) + 16) & 63
            wz = (cell + 16) & 63
            at_lane = (wx & 7) * 32 + wz
            at_row = (wx >> 3) * 32 + (wy & 3) * 8 + ((wy >> 2) & 7)
            live = slot < counts[k]
            cols.append(jnp.where(rows256 == at_lane, 1.0, 0.0).astype(BF))
            hit = rows128 == at_row
            parts = []
            for c in range(2):
                v = jnp.where(live, vals[k, pl.ds(c, 1), :], 0.0)
                for part in split(v):
                    parts.append(jnp.where(hit, part.astype(F32), 0.0).astype(BF))
            rows.append(jnp.concatenate(parts, axis=0))
        acc[...] += lax.dot_general(
            jnp.concatenate(rows, axis=1), jnp.concatenate(cols, axis=1),
            (((1,), (1,)), ((), ())), preferred_element_type=F32,
        )
        return 0

    lax.fori_loop(0, 8, place, 0)

    re = acc[0:128, :] + acc[128:256, :]
    im = acc[256:384, :] + acc[384:512, :]
    nrow = lax.broadcasted_iota(jnp.int32, (32, 128), 0)
    ny = ((nrow & 7) * 4 + (nrow >> 3) - 16).astype(F32)
    ksq = (8.0 / 4096.0) * ny * ny
    e = []
    for t in range(2):
        d = jnp.concatenate([re[:, t * 128 : t * 128 + 128], im[:, t * 128 : t * 128 + 128]], axis=1)
        dh, dl = split(d)
        e.append(dot(dh, wz_h[...]) + dot(dl, wz_h[...]) + dot(dh, wz_l[...]))

    def column(x):
        xh, t, q = x // 8, (x // 4) % 2, x % 4
        tile = e[t][xh * 32 : xh * 32 + 32, q * 128 : q * 128 + 128]
        bent = e[t][xh * 32 : xh * 32 + 32, 512 + q * 128 : 512 + q * 128 + 128]
        kin = (ksq + (8.0 / 4096.0) * (x - 16) ** 2) * tile + bent
        for j in range(4):
            ek[j, x * 8 : x * 8 + 8, :] = kin[j * 8 : j * 8 + 8, :]
        return jnp.concatenate([tile, turn * pltpu.roll(tile, 64, 1)], axis=0)

    for x in range(0, 32, 2):
        d = jnp.concatenate([column(x), column(x + 1)], axis=1)
        dh, dl = split(d)
        y = dot(ty[...], jnp.concatenate([dh, dl, dh], axis=0))
        h[x * HS : x * HS + 64, :] = y[:, 0:128]
        h[(x + 1) * HS : (x + 1) * HS + 64, :] = y[:, 128:256]

    def plane(i, _):
        both = []
        for q in range(2):
            tile = h[pl.ds(i * 2 + q, 32, stride=HS), :]
            both.append(jnp.concatenate([tile, turn * pltpu.roll(tile, 64, 1)], axis=0))
        dh, dl = split(jnp.concatenate(both, axis=1))
        real = dot(tx[...], jnp.concatenate([dh, dl, dh], axis=0))
        v = pot[i]
        vr = pltpu.roll(v, 64, 1)
        low = lane < 64
        vv = jnp.concatenate([jnp.where(low, v, vr), jnp.where(low, vr, v)], axis=1)
        dh, dl = split(real * vv)
        pq = dot(fx[...], jnp.concatenate([dh, dl, dh], axis=0))
        for q in range(2):
            p = pq[0:32, q * 128 : q * 128 + 128]
            s = pq[32:64, q * 128 : q * 128 + 128]
            start = pl.multiple_of((i * 2 + q) * FS, 8)
            f[pl.ds(start, 32), :] = p - turn * pltpu.roll(s, 64, 1)
        return 0

    lax.fori_loop(0, 32, plane, 0, unroll=4)

    def line(i, _):
        d = jnp.concatenate([f[pl.ds(i * 2 + q, 64, stride=FS), :] for q in range(2)], axis=1)
        dh, dl = split(d)
        pq = dot(fy[...], jnp.concatenate([dh, dl, dh], axis=0))
        for q in range(2):
            p = pq[0:32, q * 128 : q * 128 + 128]
            s = pq[32:64, q * 128 : q * 128 + 128]
            y = p - turn * pltpu.roll(s, 64, 1)
            start = pl.multiple_of((i * 2 + q) * 8, 8)
            for j in range(4):
                g[j, pl.ds(start, 8), :] = y[j * 8 : j * 8 + 8, :] + ek[j, pl.ds(start, 8), :]
        return 0

    lax.fori_loop(0, 16, line, 0, unroll=4)

    d = jnp.concatenate([g[j] for j in range(4)], axis=1)
    dh, dl = split(d)
    z = dot(dh, wf_h[...]) + dot(dl, wf_h[...]) + dot(dh, wf_l[...])
    for c in range(2):
        o[c] = z[:, c * 128 : c * 128 + 128]
        for b in range(8):
            out[0, c, :, b * 128 : b * 128 + 128] = o[c, pl.ds(b, 32, stride=8), :]


def apply_band(counts, vals, idx, pot):
    consts = tables()
    vm = pl.BlockSpec(memory_space=pltpu.VMEM)
    return pl.pallas_call(
        apply_kernel,
        out_shape=jax.ShapeDtypeStruct((1, 2, 32, 1024), F32),
        in_specs=[pl.BlockSpec(memory_space=pltpu.SMEM)] + [vm] * 11,
        out_specs=vm,
        scratch_shapes=[
            pltpu.VMEM((512, 256), F32),
            pltpu.VMEM((4, 256, 128), F32),
            pltpu.VMEM((32 * HS, 128), F32),
            pltpu.VMEM((64 * FS, 128), F32),
            pltpu.VMEM((4, 256, 128), F32),
            pltpu.VMEM((2, 256, 128), F32),
        ],
        compiler_params=pltpu.CompilerParams(vmem_limit_bytes=48 << 20),
        name="apply_band",
    )(counts, vals, idx, pot, *[jnp.asarray(c) for c in consts])

from jax.sharding import Mesh
from jax.sharding import PartitionSpec as P

GA = ("ga_0", "ga_1", "ga_2")
BAND = ("band_0", "band_1")
BAND_GA = ("band_0", "band_1", "ga_0", "ga_1", "ga_2")

def in_order(parts, dim):
    parts = jnp.moveaxis(parts, 0, dim)
    dims = parts.shape
    return parts.reshape(*dims[:dim], dims[dim] * dims[dim + 1], *dims[dim + 2 :])


def gather_in_order(value, axes, order):
    parts = value
    for k in order:
        parts = lax.all_gather(parts, axes[k])
    done = order[::-1]
    back = [done.index(k) for k in range(len(axes))]
    parts = parts.transpose(*back, *range(len(axes), parts.ndim))
    return parts.reshape(-1, *value.shape)


def gather_axes(value, axes, order, dim):
    return in_order(gather_in_order(value, axes, order), dim)


def cut_along(value, dim, peers):
    dims = value.shape
    parts = value.reshape(*dims[:dim], peers, dims[dim] // peers, *dims[dim + 1 :])
    return jnp.moveaxis(parts, dim, 0)


def sum_by_chip(value, chips, core, dim):
    sizes = (lax.axis_size(chips), lax.axis_size(core))
    parts = cut_along(value, dim, sizes[0] * sizes[1])
    inside = parts.shape[1:]
    parts = parts.reshape(*sizes, *inside).swapaxes(0, 1).reshape(-1, *inside)
    parts = lax.psum_scatter(parts, core, scatter_dimension=0, tiled=True)
    return lax.psum_scatter(parts, chips, scatter_dimension=0, tiled=True)[0]


def mixing(columns):
    real_cols = columns[0].T
    imag_cols = columns[1].T
    upper_rows = jnp.stack([real_cols, -imag_cols], axis=-1)
    lower_rows = jnp.stack([imag_cols, real_cols], axis=-1)
    stacked = jnp.stack([upper_rows, lower_rows], axis=1)
    return stacked.reshape(2 * real_cols.shape[0], 2 * real_cols.shape[1])


def per_device(coefficients, rotation, potential, index_map, counts):
    rot_full = gather_axes(rotation, GA, (2, 0, 1), 2)
    pot_full = gather_in_order(potential, GA, (2, 0, 1))
    band_local = coefficients.shape[0]
    slot_local = coefficients.shape[2]
    flat_coeffs = coefficients.reshape(2 * band_local, slot_local)
    product = jnp.dot(mixing(rot_full), flat_coeffs, precision=lax.Precision.HIGHEST)
    summed = sum_by_chip(
        product.reshape(rot_full.shape[2], 2, slot_local), "band_0", "band_1", 0
    )
    vals = lax.all_to_all(summed, GA, split_axis=0, concat_axis=0, tiled=True)
    return apply_band(counts, vals, index_map.reshape(32, 512), pot_full)


def solution(mesh):
    torus = Mesh(mesh.devices.reshape(4, 4, 2, 4, 2), ("ga_0", "ga_1", "ga_2", "band_0", "band_1"))
    placed = (P(BAND, None, GA), P(None, BAND, GA), P(None, GA), P(), P())
    return jax.shard_map(
        per_device,
        mesh=torus,
        in_specs=placed,
        out_specs=P(BAND_GA, None, None, None),
        check_vma=False,
    )
```

```python
import math
import numpy as np
import jax
import jax.numpy as jnp
from jax import lax
from jax.experimental import pallas as pl
from jax.experimental.pallas import tpu as pltpu
from jax.sharding import Mesh
from jax.sharding import PartitionSpec as P

F32 = jnp.float32
BF = jnp.bfloat16
HS = 72
FS = 40


def split_np(a):
    a = np.asarray(a, np.float32)
    hi = a.astype(BF)
    lo = (a - hi.astype(np.float32)).astype(BF)
    return hi, lo


def stack3(a):
    hi, lo = split_np(a)
    return np.concatenate([hi, hi, lo], axis=1)


def tables():
    n = np.arange(32) - 16
    r = np.arange(64)
    ang = 2.0 * math.pi * ((r[:, None] * n[None, :]) % 64) / 64.0
    cos, sin = np.cos(ang), np.sin(ang)
    perm = np.array([(k % 8) * 4 + k // 8 for k in range(32)])
    s = 8.0 / 4096.0
    wz = np.zeros((2, 4, 32, 2, 4, 2, 64))
    for q in range(4):
        wz[0, q, :, 0, q, 0, :] = cos.T / 64
        wz[1, q, :, 0, q, 0, :] = -sin.T / 64
        wz[0, q, :, 0, q, 1, :] = sin.T / 64
        wz[1, q, :, 0, q, 1, :] = cos.T / 64
    wz[:, :, :, 1] = wz[:, :, :, 0] * (s * n * n)[None, None, :, None, None, None]
    wz_h, wz_l = split_np(wz.reshape(256, 1024))
    ty = stack3(np.concatenate([cos[:, perm], sin[:, perm]], axis=1) / 64)
    tx = stack3(np.concatenate([cos, sin], axis=1) / 64)
    fx = stack3(np.concatenate([cos.T, sin.T], axis=0))
    fy = stack3(np.concatenate([cos.T[perm], sin.T[perm]], axis=0))
    wf = np.zeros((4, 2, 64, 2, 4, 32))
    for q in range(4):
        wf[q, 0, :, 0, q, :] = cos
        wf[q, 1, :, 0, q, :] = sin
        wf[q, 1, :, 1, q, :] = cos
        wf[q, 0, :, 1, q, :] = -sin
    wf_h, wf_l = split_np(wf.reshape(512, 256))
    return [wz_h, wz_l, ty, tx, fx, fy, wf_h, wf_l]


def split(a):
    hi = a.astype(BF)
    return hi, (a - hi.astype(F32)).astype(BF)


def dot(a, b):
    return jnp.dot(a, b, preferred_element_type=F32)


def apply_kernel(
    counts, vals, idx, pot, wz_h, wz_l, ty, tx, fx, fy, wf_h, wf_l, out,
    acc, ek, h, f, g, o,
):
    lane = lax.broadcasted_iota(jnp.int32, (1, 128), 1)
    turn = jnp.where(lane < 64, -1.0, 1.0).astype(F32)
    rows128 = lax.broadcasted_iota(jnp.int32, (128, 512), 0)
    rows256 = lax.broadcasted_iota(jnp.int32, (256, 512), 0)
    slot = lax.broadcasted_iota(jnp.int32, (1, 512), 1)

    acc[...] = jnp.zeros_like(acc)

    def place(i, _):
        cols, rows = [], []
        for q in range(4):
            k = i * 4 + q
            cell = idx[pl.ds(k, 1), :]
            wx = ((cell >> 12) + 16) & 63
            wy = ((cell >> 6) + 16) & 63
            wz = (cell + 16) & 63
            at_lane = (wx & 7) * 32 + wz
            at_row = (wx >> 3) * 32 + (wy & 3) * 8 + ((wy >> 2) & 7)
            live = slot < counts[k]
            cols.append(jnp.where(rows256 == at_lane, 1.0, 0.0).astype(BF))
            hit = rows128 == at_row
            parts = []
            for c in range(2):
                row = jnp.concatenate([vals[k, pl.ds(c * 4 + t, 1), :] for t in range(4)], axis=1)
                v = jnp.where(live, row, 0.0)
                for part in split(v):
                    parts.append(jnp.where(hit, part.astype(F32), 0.0).astype(BF))
            rows.append(jnp.concatenate(parts, axis=0))
        acc[...] += lax.dot_general(
            jnp.concatenate(rows, axis=1), jnp.concatenate(cols, axis=1),
            (((1,), (1,)), ((), ())), preferred_element_type=F32,
        )
        return 0

    lax.fori_loop(0, 8, place, 0)

    re = acc[0:128, :] + acc[128:256, :]
    im = acc[256:384, :] + acc[384:512, :]
    nrow = lax.broadcasted_iota(jnp.int32, (32, 128), 0)
    ny = ((nrow & 7) * 4 + (nrow >> 3) - 16).astype(F32)
    ksq = (8.0 / 4096.0) * ny * ny
    e = []
    for t in range(2):
        d = jnp.concatenate([re[:, t * 128 : t * 128 + 128], im[:, t * 128 : t * 128 + 128]], axis=1)
        dh, dl = split(d)
        e.append(dot(dh, wz_h[...]) + dot(dl, wz_h[...]) + dot(dh, wz_l[...]))

    def column(x):
        xh, t, q = x // 8, (x // 4) % 2, x % 4
        tile = e[t][xh * 32 : xh * 32 + 32, q * 128 : q * 128 + 128]
        bent = e[t][xh * 32 : xh * 32 + 32, 512 + q * 128 : 512 + q * 128 + 128]
        kin = (ksq + (8.0 / 4096.0) * (x - 16) ** 2) * tile + bent
        for j in range(4):
            ek[j, x * 8 : x * 8 + 8, :] = kin[j * 8 : j * 8 + 8, :]
        return jnp.concatenate([tile, turn * pltpu.roll(tile, 64, 1)], axis=0)

    for x in range(0, 32, 2):
        d = jnp.concatenate([column(x), column(x + 1)], axis=1)
        dh, dl = split(d)
        y = dot(ty[...], jnp.concatenate([dh, dl, dh], axis=0))
        h[x * HS : x * HS + 64, :] = y[:, 0:128]
        h[(x + 1) * HS : (x + 1) * HS + 64, :] = y[:, 128:256]

    def plane(i, _):
        both = []
        for q in range(2):
            tile = h[pl.ds(i * 2 + q, 32, stride=HS), :]
            both.append(jnp.concatenate([tile, turn * pltpu.roll(tile, 64, 1)], axis=0))
        dh, dl = split(jnp.concatenate(both, axis=1))
        real = dot(tx[...], jnp.concatenate([dh, dl, dh], axis=0))
        v = pot[i]
        vr = pltpu.roll(v, 64, 1)
        low = lane < 64
        vv = jnp.concatenate([jnp.where(low, v, vr), jnp.where(low, vr, v)], axis=1)
        dh, dl = split(real * vv)
        pq = dot(fx[...], jnp.concatenate([dh, dl, dh], axis=0))
        for q in range(2):
            p = pq[0:32, q * 128 : q * 128 + 128]
            s = pq[32:64, q * 128 : q * 128 + 128]
            start = pl.multiple_of((i * 2 + q) * FS, 8)
            f[pl.ds(start, 32), :] = p - turn * pltpu.roll(s, 64, 1)
        return 0

    lax.fori_loop(0, 32, plane, 0, unroll=4)

    def line(i, _):
        d = jnp.concatenate([f[pl.ds(i * 2 + q, 64, stride=FS), :] for q in range(2)], axis=1)
        dh, dl = split(d)
        pq = dot(fy[...], jnp.concatenate([dh, dl, dh], axis=0))
        for q in range(2):
            p = pq[0:32, q * 128 : q * 128 + 128]
            s = pq[32:64, q * 128 : q * 128 + 128]
            y = p - turn * pltpu.roll(s, 64, 1)
            start = pl.multiple_of((i * 2 + q) * 8, 8)
            for j in range(4):
                g[j, pl.ds(start, 8), :] = y[j * 8 : j * 8 + 8, :] + ek[j, pl.ds(start, 8), :]
        return 0

    lax.fori_loop(0, 16, line, 0, unroll=4)

    d = jnp.concatenate([g[j] for j in range(4)], axis=1)
    dh, dl = split(d)
    z = dot(dh, wf_h[...]) + dot(dl, wf_h[...]) + dot(dh, wf_l[...])
    for c in range(2):
        o[c] = z[:, c * 128 : c * 128 + 128]
        for b in range(8):
            out[0, c, :, b * 128 : b * 128 + 128] = o[c, pl.ds(b, 32, stride=8), :]


def apply_band(counts, vals, idx, pot):
    consts = tables()
    vm = pl.BlockSpec(memory_space=pltpu.VMEM)
    return pl.pallas_call(
        apply_kernel,
        out_shape=jax.ShapeDtypeStruct((1, 2, 32, 1024), F32),
        in_specs=[pl.BlockSpec(memory_space=pltpu.SMEM)] + [vm] * 11,
        out_specs=vm,
        scratch_shapes=[
            pltpu.VMEM((512, 256), F32),
            pltpu.VMEM((4, 256, 128), F32),
            pltpu.VMEM((32 * HS, 128), F32),
            pltpu.VMEM((64 * FS, 128), F32),
            pltpu.VMEM((4, 256, 128), F32),
            pltpu.VMEM((2, 256, 128), F32),
        ],
        compiler_params=pltpu.CompilerParams(vmem_limit_bytes=48 << 20),
        name="apply_band",
    )(counts, vals, idx, pot, *[jnp.asarray(c) for c in consts])


MESH = pl.DeviceIdType.MESH


def spread_kernel(
    rot, pot, coef, vals, vg,
    rg, ch, cl, sb, sr, pb, rz, ab,
    r_send, r_recv, v_send, v_recv, s_send, s_recv, z_send, z_recv, a_send, a_recv, w_send, w_recv,
):
    y, x, zh = lax.axis_index("ga_0"), lax.axis_index("ga_1"), lax.axis_index("ga_2")
    zl, core = lax.axis_index("band_0"), lax.axis_index("band_1")
    xy = y * 4 + x
    g = xy * 2 + zh
    far = xy * 2 + (1 - zh)
    half = pl.multiple_of(core * 32, 32)
    other = {"ga_2": 1 - zh}
    sibling = {"band_1": 1 - core}

    def mate(i):
        p = (xy + i) % 16
        return p, {"ga_0": p // 4, "ga_1": p % 4}

    barrier = pltpu.get_barrier_semaphore()

    def greet(i, _):
        pl.semaphore_signal(barrier, inc=1, device_id=mate(i)[1], device_id_type=MESH)
        return 0

    def hop(i, _):
        pl.semaphore_signal(barrier, inc=1, device_id={"band_0": (zl + i) % 4}, device_id_type=MESH)
        return 0

    pl.semaphore_signal(barrier, inc=1, device_id=other, device_id_type=MESH)
    lax.fori_loop(1, 16, greet, 0)
    lax.fori_loop(1, 4, hop, 0)
    pl.semaphore_signal(barrier, inc=1, device_id=sibling, device_id_type=MESH)
    pl.semaphore_wait(barrier, 20)

    def send(src, dst, send_sem, recv_sem, to):
        return pltpu.make_async_remote_copy(
            src_ref=src, dst_ref=dst, send_sem=send_sem, recv_sem=recv_sem,
            device_id=to, device_id_type=MESH,
        )

    def rot_copy(block, i, src, to):
        return send(src, rg.at[block], r_send.at[i], r_recv.at[block], to)

    def pot_copy(block, i, src, to):
        return send(src, vg.at[block, pl.ds(half, 32)], v_send.at[i], v_recv.at[block], to)

    pot_src = pot.at[pl.ds(half, 32)]
    rot_copy(g, 0, rot, other).start()

    def rot_out(i, _):
        rot_copy(g, i, rot, mate(i)[1]).start()
        return 0

    lax.fori_loop(1, 16, rot_out, 0)
    pot_copy(g, 0, pot_src, other).start()

    rg[g] = rot[...]
    vg[g, pl.ds(half, 32), :] = pot[pl.ds(half, 32), :]

    for c in range(2):
        for t in range(4):
            block = coef[pl.ds(t * 2 + c, 256, stride=8), :]
            hi, lo = split(block)
            ch[c * 256 : c * 256 + 256, t * 128 : t * 128 + 128] = hi
            cl[c * 256 : c * 256 + 256, t * 128 : t * 128 + 128] = lo

    rot_copy(far, 16, rg.at[far], other).wait_recv()

    def rot_on(i, _):
        rot_copy(far, 16 + i, rg.at[far], mate(i)[1]).start()
        return 0

    lax.fori_loop(1, 16, rot_on, 0)

    def pot_out(i, _):
        pot_copy(g, i, pot_src, mate(i)[1]).start()
        return 0

    lax.fori_loop(1, 16, pot_out, 0)
    pot_far = vg.at[far, pl.ds(half, 32)]
    pot_copy(far, 16, pot_far, other).wait_recv()

    def pot_on(i, _):
        pot_copy(far, 16 + i, pot_far, mate(i)[1]).start()
        return 0

    lax.fori_loop(1, 16, pot_on, 0)

    def rot_in(i, _):
        p, to = mate(i)
        for h in range(2):
            rot_copy(p * 2 + h, i, rot, to).wait_recv()
        return 0

    lax.fori_loop(1, 16, rot_in, 0)

    def mixer(parity):
        rows = []
        for d in range(4):
            for k in range(4):
                block = (d * 2 + parity) * 4 + k
                re, im = rg[block, 0], rg[block, 1]
                rows.append(jnp.concatenate([re, -im], axis=1))
                rows.append(jnp.concatenate([im, re], axis=1))
        lh, ll = split(jnp.concatenate(rows, axis=0))
        return dot(lh, ch[...]) + dot(ll, ch[...]) + dot(lh, cl[...])

    def pair_copy(d):
        return send(sb.at[d], sr.at[d], s_send.at[d], s_recv.at[d], sibling)

    theirs = mixer(1 - core)
    for d in range(4):
        sb[d] = theirs[d * 64 : d * 64 + 64, :]
    for d in range(4):
        pair_copy(d).start()
    mine = mixer(core)
    for d in range(4):
        pb[d] = mine[d * 64 : d * 64 + 64, :]
    for d in range(4):
        pair_copy(d).wait_recv()
        pb[d] = pb[d] + sr[d]

    def chip_copy(i):
        d = (zl + i) % 4
        return send(pb.at[d], rz.at[zl], z_send.at[i], z_recv.at[zl], {"band_0": d})

    for i in range(1, 4):
        chip_copy(i).start()
    total = pb[zl]
    for i in range(1, 4):
        s = (zl + i) % 4
        send(pb.at[s], rz.at[s], z_send.at[i], z_recv.at[s], {"band_0": s}).wait_recv()
        total = total + rz[s]

    for k in range(4):
        for c in range(2):
            for t in range(4):
                piece = total[k * 16 + c * 8 : k * 16 + c * 8 + 8, t * 128 : t * 128 + 128]
                ab[pl.ds(k * 64 + c * 4 + t, 8, stride=8), :] = piece

    def band_copy(i):
        p = (g + i) % 32
        to = {"ga_0": p // 8, "ga_1": (p // 2) % 4, "ga_2": p % 2}
        src = ab.at[pl.ds(pl.multiple_of(p * 8, 8), 8)]
        return p, to, src

    def band_out(i, _):
        p, to, src = band_copy(i)
        send(src, vals.at[g], a_send.at[i], a_recv.at[g], to).start()
        return 0

    lax.fori_loop(1, 32, band_out, 0)
    vals[g] = ab[pl.ds(pl.multiple_of(g * 8, 8), 8), :]

    def pot_in(i, _):
        p, to = mate(i)
        for h in range(2):
            pot_copy(p * 2 + h, i, pot_src, to).wait_recv()
        return 0

    lax.fori_loop(1, 16, pot_in, 0)
    swap = send(
        vg.at[:, pl.ds(half, 32)], vg.at[:, pl.ds(half, 32)], w_send, w_recv, sibling
    )
    swap.start()

    def rot_done(i, _):
        to = mate(i)[1]
        rot_copy(g, i, rot, to).wait_send()
        rot_copy(far, 16 + i, rg.at[far], to).wait_send()
        pot_copy(g, i, pot_src, to).wait_send()
        pot_copy(far, 16 + i, pot_far, to).wait_send()
        return 0

    rot_copy(g, 0, rot, other).wait_send()
    pot_copy(g, 0, pot_src, other).wait_send()
    lax.fori_loop(1, 16, rot_done, 0)
    for d in range(4):
        pair_copy(d).wait_send()
    for i in range(1, 4):
        chip_copy(i).wait_send()

    def band_in(i, _):
        p, to, src = band_copy(i)
        send(src, vals.at[p], a_send.at[i], a_recv.at[p], to).wait_recv()
        return 0

    def band_done(i, _):
        p, to, src = band_copy(i)
        send(src, vals.at[g], a_send.at[i], a_recv.at[g], to).wait_send()
        return 0

    lax.fori_loop(1, 32, band_in, 0)
    lax.fori_loop(1, 32, band_done, 0)
    swap.wait()


def spread(rot, pot, coef):
    vm = pl.BlockSpec(memory_space=pltpu.VMEM)
    sems = [pltpu.SemaphoreType.DMA((n,)) for n in (32, 32, 32, 32, 4, 4, 4, 4, 32, 32)]
    return pl.pallas_call(
        spread_kernel,
        out_shape=[
            jax.ShapeDtypeStruct((32, 8, 128), F32),
            jax.ShapeDtypeStruct((32, 64, 128), F32),
        ],
        in_specs=[vm] * 3,
        out_specs=[vm] * 2,
        scratch_shapes=[
            pltpu.VMEM((32, 2, 8, 256), F32),
            pltpu.VMEM((512, 512), BF),
            pltpu.VMEM((512, 512), BF),
            pltpu.VMEM((4, 64, 512), F32),
            pltpu.VMEM((4, 64, 512), F32),
            pltpu.VMEM((4, 64, 512), F32),
            pltpu.VMEM((4, 64, 512), F32),
            pltpu.VMEM((256, 128), F32),
        ] + sems + [pltpu.SemaphoreType.DMA, pltpu.SemaphoreType.DMA],
        compiler_params=pltpu.CompilerParams(
            vmem_limit_bytes=32 << 20, collective_id=0, has_side_effects=True
        ),
        name="spread",
    )(rot, pot, coef)


GA = ("ga_0", "ga_1", "ga_2")
BAND = ("band_0", "band_1")


def per_device(coefficients, rotation, potential, index_map, counts):
    coef = coefficients.reshape(256, 2, 4, 128).transpose(0, 2, 1, 3).reshape(2048, 128)
    vals, pot = spread(rotation.transpose(0, 2, 1), potential, coef)
    return apply_band(counts, vals, index_map.reshape(32, 512), pot)


def solution(mesh):
    torus = Mesh(mesh.devices.reshape(4, 4, 2, 4, 2), GA + BAND)
    return jax.shard_map(
        per_device,
        mesh=torus,
        in_specs=(P(BAND, None, GA), P(None, BAND, GA), P(None, GA), P(), P()),
        out_specs=P(BAND + GA, None, None, None),
        check_vma=False,
    )
```

```python
import math

import jax
import jax.numpy as jnp
import numpy as np
from jax import lax
from jax.experimental import pallas as pl
from jax.experimental.pallas import tpu as pltpu
from jax.sharding import Mesh
from jax.sharding import PartitionSpec as P

F32 = jnp.float32
BF = jnp.bfloat16
MESH = pl.DeviceIdType.MESH
GA = ("ga_0", "ga_1", "ga_2")
BAND = ("band_0", "band_1")
HS = 72
FS = 40
EARLY = 12


def split_np(a):
    a = np.asarray(a, np.float32)
    hi = a.astype(BF)
    lo = (a - hi.astype(np.float32)).astype(BF)
    return hi, lo


def stack3(a):
    hi, lo = split_np(a)
    return np.concatenate([hi, hi, lo], axis=1)


def tables():
    n = np.arange(32) - 16
    r = np.arange(64)
    ang = 2.0 * math.pi * ((r[:, None] * n[None, :]) % 64) / 64.0
    cos, sin = np.cos(ang), np.sin(ang)
    perm = np.array([(k % 8) * 4 + k // 8 for k in range(32)])
    s = 8.0 / 4096.0
    wz = np.zeros((2, 4, 32, 2, 4, 2, 64))
    for q in range(4):
        wz[0, q, :, 0, q, 0, :] = cos.T / 64
        wz[1, q, :, 0, q, 0, :] = -sin.T / 64
        wz[0, q, :, 0, q, 1, :] = sin.T / 64
        wz[1, q, :, 0, q, 1, :] = cos.T / 64
    wz[:, :, :, 1] = wz[:, :, :, 0] * (s * n * n)[None, None, :, None, None, None]
    wz_h, wz_l = split_np(wz.reshape(256, 1024))
    ty = stack3(np.concatenate([cos[:, perm], sin[:, perm]], axis=1) / 64)
    tx = stack3(np.concatenate([cos, sin], axis=1) / 64)
    fx = stack3(np.concatenate([cos.T, sin.T], axis=0))
    fy = stack3(np.concatenate([cos.T[perm], sin.T[perm]], axis=0))
    wf = np.zeros((4, 2, 64, 2, 4, 32))
    for q in range(4):
        wf[q, 0, :, 0, q, :] = cos
        wf[q, 1, :, 0, q, :] = sin
        wf[q, 1, :, 1, q, :] = cos
        wf[q, 0, :, 1, q, :] = -sin
    wf_h, wf_l = split_np(wf.reshape(512, 256))
    return [wz_h, wz_l, ty, tx, fx, fy, wf_h, wf_l]


def split(a):
    hi = a.astype(BF)
    return hi, (a - hi.astype(F32)).astype(BF)


def dot(a, b):
    return jnp.dot(a, b, preferred_element_type=F32)


def kernel(
    rot_in, pot_in, coef_in, idx_in, counts_in,
    wz_h_in, wz_l_in, ty_in, tx_in, fx_in, fy_in, wf_h_in, wf_l_in,
    out,
    rot, pot, coef, idx, counts, wz_h, wz_l, ty, tx, fx, fy, wf_h, wf_l,
    rg, vg, ch, cl, sb, sr, pb, rz, ab, vals, cols, rows, acc, ek, h, f, gz, o,
    l_sem, r_send, r_recv, v_send, v_recv, s_send, s_recv, z_send, z_recv,
    a_send, a_recv, w_send, w_recv,
):
    y, x, zh = lax.axis_index("ga_0"), lax.axis_index("ga_1"), lax.axis_index("ga_2")
    zl, core = lax.axis_index("band_0"), lax.axis_index("band_1")
    g = y * 8 + x * 2 + zh
    far = y * 8 + x * 2 + (1 - zh)
    half = pl.multiple_of(core * 32, 32)
    other = {"ga_2": 1 - zh}
    sibling = {"band_1": 1 - core}

    local = [
        pltpu.make_async_copy(a, b, l_sem.at[n])
        for n, (a, b) in enumerate([
            (rot_in.at[:, :, 0:128], rot.at[0]), (coef_in, coef), (pot_in, pot), (idx_in, idx),
            (counts_in, counts), (wz_h_in, wz_h), (wz_l_in, wz_l), (ty_in, ty),
            (tx_in, tx), (fx_in, fx), (fy_in, fy), (wf_h_in, wf_h), (wf_l_in, wf_l),
            (rot_in.at[:, :, 128:256], rot.at[1]),
        ])
    ]
    for n in (0, 13, *range(1, 13)):
        local[n].start()

    def mate(i):
        a, b = i // 4, i % 4
        yy = (y + (a ^ (a >> 1))) % 4
        xx = (x + (b ^ (b >> 1))) % 4
        return yy * 4 + xx, {"ga_0": yy, "ga_1": xx}

    barrier = pltpu.get_barrier_semaphore()

    def greet(i, _):
        pl.semaphore_signal(barrier, inc=1, device_id=mate(i)[1], device_id_type=MESH)
        return 0

    def hop(i, _):
        pl.semaphore_signal(barrier, inc=1, device_id={"band_0": (zl + i) % 4}, device_id_type=MESH)
        return 0

    pl.semaphore_signal(barrier, inc=1, device_id=other, device_id_type=MESH)
    lax.fori_loop(1, 16, greet, 0)
    lax.fori_loop(1, 4, hop, 0)
    pl.semaphore_signal(barrier, inc=1, device_id=sibling, device_id_type=MESH)

    local[0].wait()
    local[13].wait()
    for t in range(2):
        for s in range(2):
            for r in range(2):
                rg[g, s, r * 4 : r * 4 + 4, t * 128 : t * 128 + 128] = rot[
                    t, r, pl.ds(s, 4, stride=2), :
                ]
    local[2].wait()
    vg[g, pl.ds(half, 32), :] = pot[pl.ds(half, 32), :]
    pl.semaphore_wait(barrier, 20)

    def send(src, dst, send_sem, recv_sem, to):
        return pltpu.make_async_remote_copy(
            src_ref=src, dst_ref=dst, send_sem=send_sem, recv_sem=recv_sem,
            device_id=to, device_id_type=MESH,
        )

    def rot_copy(block, i, to):
        return send(rg.at[block], rg.at[block], r_send.at[i], r_recv.at[block], to)

    def pot_copy(block, i, to):
        piece = vg.at[block, pl.ds(half, 32)]
        return send(piece, piece, v_send.at[i], v_recv.at[block], to)

    def each(lo, copy):
        def step(i, _):
            copy(i).start()
            return 0

        lax.fori_loop(lo, 16, step, 0)

    rot_copy(g, 0, other).start()
    each(1, lambda i: rot_copy(g, i, mate(i)[1]))
    pot_copy(g, 0, other).start()

    local[1].wait()
    for c in range(2):
        for t in range(4):
            hi, lo = split(coef[pl.ds(t * 2 + c, 256, stride=8), :])
            ch[c * 256 : c * 256 + 256, t * 128 : t * 128 + 128] = hi
            cl[c * 256 : c * 256 + 256, t * 128 : t * 128 + 128] = lo

    local[3].wait()
    local[4].wait()
    rows128 = lax.broadcasted_iota(jnp.int32, (128, 512), 0)
    rows256 = lax.broadcasted_iota(jnp.int32, (256, 512), 0)
    slot = lax.broadcasted_iota(jnp.int32, (1, 512), 1)

    def one_hot(k, _):
        cell = jnp.concatenate([idx[pl.ds(k * 4 + t, 1), :] for t in range(4)], axis=1)
        wx = ((cell >> 12) + 16) & 63
        wy = ((cell >> 6) + 16) & 63
        wz = (cell + 16) & 63
        at_lane = (wx & 7) * 32 + wz
        at_row = (wx >> 3) * 32 + (wy & 3) * 8 + ((wy >> 2) & 7)
        at_row = jnp.where(slot < counts[k], at_row, -1)
        cols[k] = jnp.where(rows256 == at_lane, 1.0, 0.0).astype(BF)
        rows[k] = jnp.where(rows128 == at_row, 1.0, 0.0).astype(BF)
        return 0

    lax.fori_loop(0, EARLY, one_hot, 0)

    rot_copy(far, 16, other).wait_recv()
    each(1, lambda i: rot_copy(far, 16 + i, mate(i)[1]))
    each(1, lambda i: pot_copy(g, i, mate(i)[1]))
    pot_copy(far, 16, other).wait_recv()
    each(1, lambda i: pot_copy(far, 16 + i, mate(i)[1]))

    lax.fori_loop(EARLY, 32, one_hot, 0)

    sub = lax.broadcasted_iota(jnp.int32, (8, 256), 0)
    flip = jnp.where(sub < 4, -1.0, 1.0).astype(F32)

    def pair_copy(d):
        return send(sb.at[d], sr.at[d], s_send.at[d], s_recv.at[d], sibling)

    def chip_copy(d, part, to, place):
        return send(
            pb.at[d, pl.ds(part * 32, 32)], rz.at[part, place],
            z_send.at[part * 4 + d], z_recv.at[part * 5 + place], {"band_0": to},
        )

    def mix(n):
        d = (y + (n ^ (n >> 1))) % 4

        def rot_wait(i, _):
            p, to = mate(i)
            rot_copy(p * 2, 0, to).wait_recv()
            rot_copy(p * 2 + 1, 0, to).wait_recv()
            return 0

        lax.fori_loop(max(1, n * 4), n * 4 + 4, rot_wait, 0)
        left, right = [], []
        for parity in (1 - core, core):
            for s in (1 - zh, zh):
                for k in range(4):
                    block = rg[d * 8 + parity * 4 + k, s]
                    left.append(block)
                    right.append(flip * pltpu.roll(block, 4, 0))
        lh, ll = split(jnp.concatenate([jnp.concatenate(left, 0), jnp.concatenate(right, 0)], 1))
        both = dot(lh, ch[...]) + dot(ll, ch[...]) + dot(lh, cl[...])
        sb[d] = both[0:64]
        pb[d] = both[64:128]
        pair_copy(d).start()

    def scatter_half(n, part):
        d = (y + (n ^ (n >> 1))) % 4
        up = (zl == 0) & (d == 2)
        down = (zl == 3) & (d == 1)
        wait_for = ((zl == 1) & (d == 2)) | ((zl == 2) & (d == 1))

        @pl.when((d != zl) & jnp.logical_not(wait_for))
        def _():
            to = jnp.where(up, 1, jnp.where(down, 2, d))
            place = jnp.where(up | down, 4, zl)
            chip_copy(d, part, to, place).start()

    def settle(n):
        d = (y + (n ^ (n >> 1))) % 4
        pair_copy(d).wait_recv()
        pb[d] = pb[d] + sr[d]
        scatter_half(n, 0)

    mix(0)
    for n in range(1, 4):
        mix(n)
        settle(n - 1)
    settle(3)

    def merge(part):
        @pl.when((zl == 1) | (zl == 2))
        def _():
            d = 3 - zl
            chip_copy(d, part, d, 4).wait_recv()
            pb[d, part * 32 : part * 32 + 32] = pb[d, part * 32 : part * 32 + 32] + rz[part, 4]
            chip_copy(d, part, d, zl).start()

    def band_copy(p, part, to):
        s = (1 - zh) if part == 0 else zh
        gg = p * 2 + s
        src = ab.at[pl.ds(pl.multiple_of(gg * 8, 8), 8)]
        return send(src, vals.at[g], a_send.at[gg], a_recv.at[g], {**to, "ga_2": s})

    def finish(part):
        s = (1 - zh) if part == 0 else zh
        for src in range(4):
            skip = (zl == src) | ((zl == 2) & (src == 0)) | ((zl == 1) & (src == 3))

            @pl.when(jnp.logical_not(skip))
            def _():
                chip_copy(zl, part, zl, src).wait_recv()
                pb[zl, part * 32 : part * 32 + 32] = (
                    pb[zl, part * 32 : part * 32 + 32] + rz[part, src]
                )

        total = pb[zl, part * 32 : part * 32 + 32]
        for k in range(4):
            for c in range(2):
                for t in range(4):
                    piece = total[k * 8 + c * 4 : k * 8 + c * 4 + 4, t * 128 : t * 128 + 128]
                    ab[pl.ds(k * 64 + s * 8 + c * 4 + t, 4, stride=16), :] = piece

        def out_step(i, _):
            p, to = mate(15 - i)
            band_copy(p, part, to).start()
            return 0

        lax.fori_loop(0, 16 - part, out_step, 0)

    merge(0)
    for n in range(4):
        scatter_half(n, 1)
    finish(0)
    merge(1)
    finish(1)
    vals[g] = ab[pl.ds(pl.multiple_of(g * 8, 8), 8), :]

    def pot_wait(i, _):
        p, to = mate(i)
        pot_copy(p * 2, 0, to).wait_recv()
        pot_copy(p * 2 + 1, 0, to).wait_recv()
        return 0

    lax.fori_loop(1, 16, pot_wait, 0)
    side = vg.at[:, pl.ds(half, 32)]
    swap = send(side, side, w_send, w_recv, sibling)
    swap.start()

    def place(i, first=False):
        p, to = mate(i)
        if first:
            send(ab.at[pl.ds(0, 8)], vals.at[far], a_send.at[0], a_recv.at[far], to).wait_recv()
        else:
            for q in range(2):
                k = p * 2 + q
                send(ab.at[pl.ds(0, 8)], vals.at[k], a_send.at[0], a_recv.at[k], to).wait_recv()
        left = []
        for q in range(2):
            k = p * 2 + q
            hit = rows[k]
            parts = []
            for c in range(2):
                v = jnp.concatenate([vals[k, pl.ds(c * 4 + t, 1), :] for t in range(4)], axis=1)
                high = v.astype(BF).astype(F32)
                for part in (high, v - high):
                    wide = jnp.broadcast_to(part, (16, 512)).astype(BF)
                    parts.append(hit * jnp.concatenate([wide] * 8, axis=0))
            left.append(jnp.concatenate(parts, axis=0))
        right = jnp.concatenate([cols[p * 2], cols[p * 2 + 1]], axis=1)
        placed = lax.dot_general(
            jnp.concatenate(left, axis=1), right, (((1,), (1,)), ((), ())),
            preferred_element_type=F32,
        )
        if first:
            acc[...] = placed
        else:
            acc[...] += placed

    place(0, True)

    def place_step(i, _):
        place(i)
        return 0

    lax.fori_loop(1, 16, place_step, 0)

    for copy in local[5:13]:
        copy.wait()
    lane = lax.broadcasted_iota(jnp.int32, (1, 128), 1)
    turn = jnp.where(lane < 64, -1.0, 1.0).astype(F32)
    re = acc[0:128, :] + acc[128:256, :]
    im = acc[256:384, :] + acc[384:512, :]
    nrow = lax.broadcasted_iota(jnp.int32, (32, 128), 0)
    ny = ((nrow & 7) * 4 + (nrow >> 3) - 16).astype(F32)
    ksq = (8.0 / 4096.0) * ny * ny
    e = []
    for t in range(2):
        d = jnp.concatenate([re[:, t * 128 : t * 128 + 128], im[:, t * 128 : t * 128 + 128]], axis=1)
        dh, dl = split(d)
        e.append(dot(dh, wz_h[...]) + dot(dl, wz_h[...]) + dot(dh, wz_l[...]))

    def column(i):
        xh, t, q = i // 8, (i // 4) % 2, i % 4
        tile = e[t][xh * 32 : xh * 32 + 32, q * 128 : q * 128 + 128]
        bent = e[t][xh * 32 : xh * 32 + 32, 512 + q * 128 : 512 + q * 128 + 128]
        kin = (ksq + (8.0 / 4096.0) * (i - 16) ** 2) * tile + bent
        for j in range(4):
            ek[j, i * 8 : i * 8 + 8, :] = kin[j * 8 : j * 8 + 8, :]
        return jnp.concatenate([tile, turn * pltpu.roll(tile, 64, 1)], axis=0)

    for i in range(0, 32, 2):
        dh, dl = split(jnp.concatenate([column(i), column(i + 1)], axis=1))
        d = dot(ty[...], jnp.concatenate([dh, dl, dh], axis=0))
        h[i * HS : i * HS + 64, :] = d[:, 0:128]
        h[(i + 1) * HS : (i + 1) * HS + 64, :] = d[:, 128:256]

    swap.wait()

    def plane(i, _):
        both = []
        for q in range(2):
            tile = h[pl.ds(i * 2 + q, 32, stride=HS), :]
            both.append(jnp.concatenate([tile, turn * pltpu.roll(tile, 64, 1)], axis=0))
        dh, dl = split(jnp.concatenate(both, axis=1))
        real = dot(tx[...], jnp.concatenate([dh, dl, dh], axis=0))
        v = vg[i]
        vr = pltpu.roll(v, 64, 1)
        low = lane < 64
        vv = jnp.concatenate([jnp.where(low, v, vr), jnp.where(low, vr, v)], axis=1)
        dh, dl = split(real * vv)
        pq = dot(fx[...], jnp.concatenate([dh, dl, dh], axis=0))
        for q in range(2):
            pp = pq[0:32, q * 128 : q * 128 + 128]
            qq = pq[32:64, q * 128 : q * 128 + 128]
            start = pl.multiple_of((i * 2 + q) * FS, 8)
            f[pl.ds(start, 32), :] = pp - turn * pltpu.roll(qq, 64, 1)
        return 0

    lax.fori_loop(0, 32, plane, 0, unroll=16)

    def line(i, _):
        d = jnp.concatenate([f[pl.ds(i * 2 + q, 64, stride=FS), :] for q in range(2)], axis=1)
        dh, dl = split(d)
        pq = dot(fy[...], jnp.concatenate([dh, dl, dh], axis=0))
        for q in range(2):
            pp = pq[0:32, q * 128 : q * 128 + 128]
            qq = pq[32:64, q * 128 : q * 128 + 128]
            yy = pp - turn * pltpu.roll(qq, 64, 1)
            start = pl.multiple_of((i * 2 + q) * 8, 8)
            for j in range(4):
                gz[j, pl.ds(start, 8), :] = yy[j * 8 : j * 8 + 8, :] + ek[j, pl.ds(start, 8), :]
        return 0

    lax.fori_loop(0, 16, line, 0, unroll=16)

    dh, dl = split(jnp.concatenate([gz[j] for j in range(4)], axis=1))
    z = dot(dh, wf_h[...]) + dot(dl, wf_h[...]) + dot(dh, wf_l[...])
    for c in range(2):
        o[c] = z[:, c * 128 : c * 128 + 128]
        for b in range(8):
            out[0, c, :, b * 128 : b * 128 + 128] = o[c, pl.ds(b, 32, stride=8), :]

    rot_copy(g, 0, other).wait_send()
    pot_copy(g, 0, other).wait_send()

    def sent(i, _):
        to = mate(i)[1]
        rot_copy(g, i, to).wait_send()
        rot_copy(far, 16 + i, to).wait_send()
        pot_copy(g, i, to).wait_send()
        pot_copy(far, 16 + i, to).wait_send()
        return 0

    lax.fori_loop(1, 16, sent, 0)
    for d in range(4):
        pair_copy(d).wait_send()

        @pl.when(zl != d)
        def _():
            chip_copy(d, 0, d, 0).wait_send()
            chip_copy(d, 1, d, 0).wait_send()

    def given(i, _):
        p, to = mate(i)
        band_copy(p, 0, to).wait_send()

        @pl.when(i > 0)
        def _():
            band_copy(p, 1, to).wait_send()

        return 0

    lax.fori_loop(0, 16, given, 0)


def run(rot, pot, coef, idx, counts):
    consts = [jnp.asarray(c) for c in tables()]
    hbm = pl.BlockSpec(memory_space=pltpu.HBM)
    sems = [pltpu.SemaphoreType.DMA((n,)) for n in (14, 32, 32, 32, 32, 4, 4, 8, 10, 32, 32)]
    return pl.pallas_call(
        kernel,
        out_shape=jax.ShapeDtypeStruct((1, 2, 32, 1024), F32),
        in_specs=[hbm] * 13,
        out_specs=pl.BlockSpec(memory_space=pltpu.VMEM),
        scratch_shapes=[
            pltpu.VMEM((2, 2, 8, 128), F32),
            pltpu.VMEM((64, 128), F32),
            pltpu.VMEM((2048, 128), F32),
            pltpu.VMEM((128, 128), jnp.int32),
            pltpu.SMEM((32,), jnp.int32),
        ] + [pltpu.VMEM(c.shape, c.dtype) for c in consts] + [
            pltpu.VMEM((32, 2, 8, 256), F32),
            pltpu.VMEM((32, 64, 128), F32),
            pltpu.VMEM((512, 512), BF),
            pltpu.VMEM((512, 512), BF),
            pltpu.VMEM((4, 64, 512), F32),
            pltpu.VMEM((4, 64, 512), F32),
            pltpu.VMEM((4, 64, 512), F32),
            pltpu.VMEM((2, 5, 32, 512), F32),
            pltpu.VMEM((256, 128), F32),
            pltpu.VMEM((32, 8, 128), F32),
            pltpu.VMEM((32, 256, 512), BF),
            pltpu.VMEM((32, 128, 512), BF),
            pltpu.VMEM((512, 256), F32),
            pltpu.VMEM((4, 256, 128), F32),
            pltpu.VMEM((32 * HS, 128), F32),
            pltpu.VMEM((64 * FS, 128), F32),
            pltpu.VMEM((4, 256, 128), F32),
            pltpu.VMEM((2, 256, 128), F32),
        ] + sems + [pltpu.SemaphoreType.DMA, pltpu.SemaphoreType.DMA],
        compiler_params=pltpu.CompilerParams(
            vmem_limit_bytes=56 << 20, collective_id=0, has_side_effects=True
        ),
        name="panel",
    )(rot, pot, coef, idx, counts, *consts)


def per_device(coefficients, rotation, potential, index_map, counts):
    coef = coefficients.reshape(256, 2, 4, 128).transpose(0, 2, 1, 3).reshape(2048, 128)
    return run(
        rotation.transpose(0, 2, 1), potential, coef, index_map.reshape(128, 128), counts
    )


def solution(mesh):
    torus = Mesh(mesh.devices.reshape(4, 4, 2, 4, 2), GA + BAND)
    return jax.shard_map(
        per_device,
        mesh=torus,
        in_specs=(P(BAND, None, GA), P(None, BAND, GA), P(None, GA), P(), P()),
        out_specs=P(BAND + GA, None, None, None),
        check_vma=False,
    )
```

```python
import math

import jax
import jax.numpy as jnp
import numpy as np
from jax import lax
from jax.experimental import pallas as pl
from jax.experimental.pallas import tpu as pltpu
from jax.sharding import Mesh
from jax.sharding import PartitionSpec as P

F32 = jnp.float32
BF = jnp.bfloat16
MESH = pl.DeviceIdType.MESH
GA = ("ga_0", "ga_1", "ga_2")
BAND = ("band_0", "band_1")
HS = 72
FS = 40


def split_np(a):
    a = np.asarray(a, np.float32)
    hi = a.astype(BF)
    lo = (a - hi.astype(np.float32)).astype(BF)
    return hi, lo


def stack3(a):
    hi, lo = split_np(a)
    return np.concatenate([hi, hi, lo], axis=1)


def tables():
    n = np.arange(32) - 16
    r = np.arange(64)
    ang = 2.0 * math.pi * ((r[:, None] * n[None, :]) % 64) / 64.0
    cos, sin = np.cos(ang), np.sin(ang)
    perm = np.array([(k % 8) * 4 + k // 8 for k in range(32)])
    s = 8.0 / 4096.0
    wz = np.zeros((2, 4, 32, 2, 4, 2, 64))
    for q in range(4):
        wz[0, q, :, 0, q, 0, :] = cos.T / 64
        wz[1, q, :, 0, q, 0, :] = -sin.T / 64
        wz[0, q, :, 0, q, 1, :] = sin.T / 64
        wz[1, q, :, 0, q, 1, :] = cos.T / 64
    wz[:, :, :, 1] = wz[:, :, :, 0] * (s * n * n)[None, None, :, None, None, None]
    wz_h, wz_l = split_np(wz.reshape(256, 1024))
    ty = stack3(np.concatenate([cos[:, perm], sin[:, perm]], axis=1) / 64)
    tx = stack3(np.concatenate([cos, sin], axis=1) / 64)
    fx = stack3(np.concatenate([cos.T, sin.T], axis=0))
    fy = stack3(np.concatenate([cos.T[perm], sin.T[perm]], axis=0))
    wf = np.zeros((4, 2, 64, 2, 4, 32))
    for q in range(4):
        wf[q, 0, :, 0, q, :] = cos
        wf[q, 1, :, 0, q, :] = sin
        wf[q, 1, :, 1, q, :] = cos
        wf[q, 0, :, 1, q, :] = -sin
    wf_h, wf_l = split_np(wf.reshape(512, 256))
    return [wz_h, wz_l, ty, tx, fx, fy, wf_h, wf_l]


def split(a):
    hi = a.astype(BF)
    return hi, (a - hi.astype(F32)).astype(BF)


def dot(a, b):
    return jnp.dot(a, b, preferred_element_type=F32)


def kernel(
    rot_in, pot_in, coef_in, idx_in, counts_in,
    wz_h_in, wz_l_in, ty_in, tx_in, fx_in, fy_in, wf_h_in, wf_l_in,
    out,
    rot, pot, coef, idx, counts, wz_h, wz_l, ty, tx, fx, fy, wf_h, wf_l,
    rg, vg, ch, cl, sb, sr, pb, rz, ab, vals, cols, rows, acc, ek, h, f, gz, o,
    l_sem, r_send, r_recv, v_send, v_recv, s_send, s_recv, z_send, z_recv,
    a_send, a_recv, w_send, w_recv,
):
    y, x, zh = lax.axis_index("ga_0"), lax.axis_index("ga_1"), lax.axis_index("ga_2")
    zl, core = lax.axis_index("band_0"), lax.axis_index("band_1")
    g = y * 8 + x * 2 + zh
    far = y * 8 + x * 2 + (1 - zh)
    half = pl.multiple_of(core * 32, 32)
    other = {"ga_2": 1 - zh}
    sibling = {"band_1": 1 - core}

    local = [
        pltpu.make_async_copy(a, b, l_sem.at[n])
        for n, (a, b) in enumerate([
            (rot_in.at[:, :, 0:128], rot.at[0]), (coef_in, coef), (pot_in, pot), (idx_in, idx),
            (counts_in, counts), (wz_h_in, wz_h), (wz_l_in, wz_l), (ty_in, ty),
            (tx_in, tx), (fx_in, fx), (fy_in, fy), (wf_h_in, wf_h), (wf_l_in, wf_l),
            (rot_in.at[:, :, 128:256], rot.at[1]),
        ])
    ]
    for n in (0, 13, *range(1, 13)):
        local[n].start()

    def mate(i):
        a, b = i // 4, i % 4
        yy = (y + (a ^ (a >> 1))) % 4
        xx = (x + (b ^ (b >> 1))) % 4
        return yy * 4 + xx, {"ga_0": yy, "ga_1": xx}

    barrier = pltpu.get_barrier_semaphore()

    def greet(i, _):
        pl.semaphore_signal(barrier, inc=1, device_id=mate(i)[1], device_id_type=MESH)
        return 0

    def hop(i, _):
        pl.semaphore_signal(barrier, inc=1, device_id={"band_0": (zl + i) % 4}, device_id_type=MESH)
        return 0

    pl.semaphore_signal(barrier, inc=1, device_id=other, device_id_type=MESH)
    lax.fori_loop(1, 16, greet, 0)
    lax.fori_loop(1, 4, hop, 0)
    pl.semaphore_signal(barrier, inc=1, device_id=sibling, device_id_type=MESH)

    local[0].wait()
    local[13].wait()
    for t in range(2):
        for s in range(2):
            for r in range(2):
                rg[g, s, r * 4 : r * 4 + 4, t * 128 : t * 128 + 128] = rot[
                    t, r, pl.ds(s, 4, stride=2), :
                ]
    local[2].wait()
    vg[g, pl.ds(half, 32), :] = pot[pl.ds(half, 32), :]
    pl.semaphore_wait(barrier, 20)

    def send(src, dst, send_sem, recv_sem, to):
        return pltpu.make_async_remote_copy(
            src_ref=src, dst_ref=dst, send_sem=send_sem, recv_sem=recv_sem,
            device_id=to, device_id_type=MESH,
        )

    def rot_copy(block, i, to):
        return send(rg.at[block], rg.at[block], r_send.at[i], r_recv.at[block], to)

    def pot_copy(block, i, to):
        piece = vg.at[block, pl.ds(half, 32)]
        return send(piece, piece, v_send.at[i], v_recv.at[block], to)

    def each(lo, copy):
        def step(i, _):
            copy(i).start()
            return 0

        lax.fori_loop(lo, 16, step, 0)

    rot_copy(g, 0, other).start()
    each(1, lambda i: rot_copy(g, i, mate(i)[1]))
    pot_copy(g, 0, other).start()

    local[1].wait()
    for c in range(2):
        for t in range(4):
            hi, lo = split(coef[pl.ds(t * 2 + c, 256, stride=8), :])
            ch[c * 256 : c * 256 + 256, t * 128 : t * 128 + 128] = hi
            cl[c * 256 : c * 256 + 256, t * 128 : t * 128 + 128] = lo

    local[3].wait()
    local[4].wait()
    rows128 = lax.broadcasted_iota(jnp.int32, (128, 512), 0)
    rows256 = lax.broadcasted_iota(jnp.int32, (256, 512), 0)
    slot = lax.broadcasted_iota(jnp.int32, (1, 512), 1)

    def one_hot(k, _):
        cell = jnp.concatenate([idx[pl.ds(k * 4 + t, 1), :] for t in range(4)], axis=1)
        wx = ((cell >> 12) + 16) & 63
        wy = ((cell >> 6) + 16) & 63
        wz = (cell + 16) & 63
        at_lane = (wx & 7) * 32 + wz
        at_row = (wx >> 3) * 32 + (wy & 3) * 8 + ((wy >> 2) & 7)
        at_row = jnp.where(slot < counts[k], at_row, -1)
        cols[k] = jnp.where(rows256 == at_lane, 1.0, 0.0).astype(BF)
        rows[k] = jnp.where(rows128 == at_row, 1.0, 0.0).astype(BF)
        return 0

    sub = lax.broadcasted_iota(jnp.int32, (8, 256), 0)
    flip = jnp.where(sub < 4, -1.0, 1.0).astype(F32)

    def row_of(n):
        return (y + (n ^ (n >> 1))) % 4

    def plane_of(q):
        return zh if q == 0 else 1 - zh

    def pair_copy(q, d):
        return send(sb.at[q, d], sr.at[q, d], s_send.at[q * 4 + d], s_recv.at[q * 4 + d], sibling)

    def chip_copy(q, d, away, src):
        to = {"band_0": d, "ga_2": 1 - zh} if away else {"band_0": d}
        return send(
            pb.at[q, d, pl.ds(away * 16, 16)], rz.at[q, away, src],
            z_send.at[q * 8 + d * 2 + away], z_recv.at[q * 8 + src * 2 + away], to,
        )

    def mix(q, n):
        d = row_of(n)

        def rot_wait(i, _):
            p, to = mate(i)
            rot_copy(p * 2 + plane_of(q), 0, to).wait_recv()
            return 0

        lax.fori_loop(max(1, n * 4), n * 4 + 4, rot_wait, 0)
        left, right = [], []
        for parity in (1 - core, core):
            for t in (zh, 1 - zh):
                for xb in range(2):
                    block = rg[d * 8 + (parity * 2 + xb) * 2 + plane_of(q), t]
                    left.append(block)
                    right.append(flip * pltpu.roll(block, 4, 0))
        lh, ll = split(jnp.concatenate([jnp.concatenate(left, 0), jnp.concatenate(right, 0)], 1))
        high = dot(jnp.concatenate([lh, ll], axis=0), ch[...])
        both = high[0:64] + high[64:128] + dot(lh, cl[...])
        sb[q, d] = both[0:32]
        pb[q, d] = both[32:64]
        pair_copy(q, d).start()

    def settle(q, n):
        d = row_of(n)
        pair_copy(q, d).wait_recv()
        pb[q, d] = pb[q, d] + sr[q, d]
        chip_copy(q, d, 1, zl).start()

        @pl.when(d != zl)
        def _():
            chip_copy(q, d, 0, zl).start()

    def band_copy(q, i):
        away, xb, xx = 1 - i // 8, (i // 4) % 2, (x + 3 - i % 4) % 4
        source = plane_of(away)
        yy = xb * 2 + plane_of(q ^ away)
        slot16 = yy * 4 + xx
        src = ab.at[pl.ds(pl.multiple_of(away * 128 + slot16 * 8, 8), 8)]
        block = (y * 4 + x) * 2 + source
        to = {"ga_0": yy, "ga_1": xx}
        return slot16, send(
            src, vals.at[block], a_send.at[away * 16 + slot16], a_recv.at[block], to
        )

    def finish(q):
        for away in (1, 0):
            total = pb[q, zl, 0:16, :] if away == 0 else None
            for i in range(1 - away, 4):
                src = (zl + i) % 4
                chip_copy(q, zl, away, src).wait_recv()
                part = rz[q, away, src]
                total = part if total is None else total + part
            for xb in range(2):
                for c in range(2):
                    for t in range(4):
                        start = away * 128 + (xb * 2 + plane_of(q ^ away)) * 32 + c * 4 + t
                        at = xb * 8 + c * 4
                        ab[pl.ds(start, 4, stride=8), :] = total[at : at + 4, t * 128 : t * 128 + 128]
            for i in range(8):
                slot16, copy = band_copy(q, i + 8 * (1 - away))

                @pl.when(slot16 != y * 4 + x)
                def _():
                    copy.start()

    lax.fori_loop(0, 32, one_hot, 0)
    mix(0, 0)
    rot_copy(far, 16, other).wait_recv()
    each(1, lambda i: rot_copy(far, 16 + i, mate(i)[1]))
    settle(0, 0)
    mix(0, 1)
    mix(0, 2)
    settle(0, 1)
    each(1, lambda i: pot_copy(g, i, mate(i)[1]))
    mix(0, 3)
    settle(0, 2)
    mix(1, 0)
    settle(0, 3)
    mix(1, 1)
    settle(1, 0)
    mix(1, 2)
    settle(1, 1)
    mix(1, 3)
    settle(1, 2)
    settle(1, 3)
    pot_copy(far, 16, other).wait_recv()
    each(1, lambda i: pot_copy(far, 16 + i, mate(i)[1]))
    finish(0)
    finish(1)
    home = pl.multiple_of((y * 4 + x) * 8, 8)
    vals[g] = ab[pl.ds(home, 8), :]
    vals[far] = ab[pl.ds(home + 128, 8), :]

    def place(i, plane):
        left, right = [], []
        for b in range(4):
            p, to = mate(i * 4 + b)
            k = p * 2 + plane

            @pl.when(p != y * 4 + x)
            def _():
                send(ab.at[pl.ds(0, 8)], vals.at[k], a_send.at[0], a_recv.at[k], to).wait_recv()

        for b in range(4):
            k = mate(i * 4 + b)[0] * 2 + plane
            hit = rows[k]
            parts = []
            for c in range(2):
                v = jnp.concatenate([vals[k, pl.ds(c * 4 + t, 1), :] for t in range(4)], axis=1)
                high = v.astype(BF).astype(F32)
                for part in (high, v - high):
                    wide = jnp.broadcast_to(part, (16, 512)).astype(BF)
                    parts.append(hit * jnp.concatenate([wide] * 8, axis=0))
            left.append(jnp.concatenate(parts, axis=0))
            right.append(cols[k])
        return lax.dot_general(
            jnp.concatenate(left, axis=1), jnp.concatenate(right, axis=1),
            (((1,), (1,)), ((), ())), preferred_element_type=F32,
        )

    soon = y % 2
    acc[...] = place(0, soon)

    def place_soon(i, _):
        acc[...] += place(i, soon)
        return 0

    def place_late(i, _):
        acc[...] += place(i, 1 - soon)
        return 0

    lax.fori_loop(1, 4, place_soon, 0)

    def pot_wait(i, _):
        p, to = mate(i)
        pot_copy(p * 2, 0, to).wait_recv()
        pot_copy(p * 2 + 1, 0, to).wait_recv()
        return 0

    lax.fori_loop(1, 16, pot_wait, 0)
    side = vg.at[:, pl.ds(half, 32)]
    swap = send(side, side, w_send, w_recv, sibling)
    swap.start()
    lax.fori_loop(0, 4, place_late, 0)

    for copy in local[5:13]:
        copy.wait()
    lane = lax.broadcasted_iota(jnp.int32, (1, 128), 1)
    turn = jnp.where(lane < 64, -1.0, 1.0).astype(F32)
    re = acc[0:128, :] + acc[128:256, :]
    im = acc[256:384, :] + acc[384:512, :]
    nrow = lax.broadcasted_iota(jnp.int32, (32, 128), 0)
    ny = ((nrow & 7) * 4 + (nrow >> 3) - 16).astype(F32)
    ksq = (8.0 / 4096.0) * ny * ny
    e = []
    for t in range(2):
        d = jnp.concatenate([re[:, t * 128 : t * 128 + 128], im[:, t * 128 : t * 128 + 128]], axis=1)
        dh, dl = split(d)
        e.append(dot(dh, wz_h[...]) + dot(dl, wz_h[...]) + dot(dh, wz_l[...]))

    def column(i):
        xh, t, q = i // 8, (i // 4) % 2, i % 4
        tile = e[t][xh * 32 : xh * 32 + 32, q * 128 : q * 128 + 128]
        bent = e[t][xh * 32 : xh * 32 + 32, 512 + q * 128 : 512 + q * 128 + 128]
        kin = (ksq + (8.0 / 4096.0) * (i - 16) ** 2) * tile + bent
        for j in range(4):
            ek[j, i * 8 : i * 8 + 8, :] = kin[j * 8 : j * 8 + 8, :]
        return jnp.concatenate([tile, turn * pltpu.roll(tile, 64, 1)], axis=0)

    for i in range(0, 32, 2):
        dh, dl = split(jnp.concatenate([column(i), column(i + 1)], axis=1))
        d = dot(ty[...], jnp.concatenate([dh, dl, dh], axis=0))
        h[i * HS : i * HS + 64, :] = d[:, 0:128]
        h[(i + 1) * HS : (i + 1) * HS + 64, :] = d[:, 128:256]

    swap.wait()

    def plane(i, _):
        both = []
        for q in range(2):
            tile = h[pl.ds(i * 2 + q, 32, stride=HS), :]
            both.append(jnp.concatenate([tile, turn * pltpu.roll(tile, 64, 1)], axis=0))
        dh, dl = split(jnp.concatenate(both, axis=1))
        real = dot(tx[...], jnp.concatenate([dh, dl, dh], axis=0))
        v = vg[i]
        vr = pltpu.roll(v, 64, 1)
        low = lane < 64
        vv = jnp.concatenate([jnp.where(low, v, vr), jnp.where(low, vr, v)], axis=1)
        dh, dl = split(real * vv)
        pq = dot(fx[...], jnp.concatenate([dh, dl, dh], axis=0))
        for q in range(2):
            pp = pq[0:32, q * 128 : q * 128 + 128]
            qq = pq[32:64, q * 128 : q * 128 + 128]
            start = pl.multiple_of((i * 2 + q) * FS, 8)
            f[pl.ds(start, 32), :] = pp - turn * pltpu.roll(qq, 64, 1)
        return 0

    lax.fori_loop(0, 32, plane, 0, unroll=16)

    def line(i, _):
        d = jnp.concatenate([f[pl.ds(i * 2 + q, 64, stride=FS), :] for q in range(2)], axis=1)
        dh, dl = split(d)
        pq = dot(fy[...], jnp.concatenate([dh, dl, dh], axis=0))
        for q in range(2):
            pp = pq[0:32, q * 128 : q * 128 + 128]
            qq = pq[32:64, q * 128 : q * 128 + 128]
            yy = pp - turn * pltpu.roll(qq, 64, 1)
            start = pl.multiple_of((i * 2 + q) * 8, 8)
            for j in range(4):
                gz[j, pl.ds(start, 8), :] = yy[j * 8 : j * 8 + 8, :] + ek[j, pl.ds(start, 8), :]
        return 0

    lax.fori_loop(0, 16, line, 0, unroll=16)

    dh, dl = split(jnp.concatenate([gz[j] for j in range(4)], axis=1))
    z = dot(dh, wf_h[...]) + dot(dl, wf_h[...]) + dot(dh, wf_l[...])
    for c in range(2):
        o[c] = z[:, c * 128 : c * 128 + 128]
        for b in range(8):
            out[0, c, :, b * 128 : b * 128 + 128] = o[c, pl.ds(b, 32, stride=8), :]

    rot_copy(g, 0, other).wait_send()
    pot_copy(g, 0, other).wait_send()

    def sent(i, _):
        to = mate(i)[1]
        rot_copy(g, i, to).wait_send()
        rot_copy(far, 16 + i, to).wait_send()
        pot_copy(g, i, to).wait_send()
        pot_copy(far, 16 + i, to).wait_send()
        return 0

    lax.fori_loop(1, 16, sent, 0)
    for q in range(2):
        for d in range(4):
            pair_copy(q, d).wait_send()
            chip_copy(q, d, 1, 0).wait_send()

            @pl.when(zl != d)
            def _():
                chip_copy(q, d, 0, 0).wait_send()

        for i in range(16):
            slot16, copy = band_copy(q, i)

            @pl.when(slot16 != y * 4 + x)
            def _():
                copy.wait_send()


def run(rot, pot, coef, idx, counts):
    consts = [jnp.asarray(c) for c in tables()]
    hbm = pl.BlockSpec(memory_space=pltpu.HBM)
    sems = [pltpu.SemaphoreType.DMA((n,)) for n in (14, 32, 32, 32, 32, 8, 8, 16, 16, 32, 32)]
    return pl.pallas_call(
        kernel,
        out_shape=jax.ShapeDtypeStruct((1, 2, 32, 1024), F32),
        in_specs=[hbm] * 13,
        out_specs=pl.BlockSpec(memory_space=pltpu.VMEM),
        scratch_shapes=[
            pltpu.VMEM((2, 2, 8, 128), F32),
            pltpu.VMEM((64, 128), F32),
            pltpu.VMEM((2048, 128), F32),
            pltpu.VMEM((128, 128), jnp.int32),
            pltpu.SMEM((32,), jnp.int32),
        ] + [pltpu.VMEM(c.shape, c.dtype) for c in consts] + [
            pltpu.VMEM((32, 2, 8, 256), F32),
            pltpu.VMEM((32, 64, 128), F32),
            pltpu.VMEM((512, 512), BF),
            pltpu.VMEM((512, 512), BF),
            pltpu.VMEM((2, 4, 32, 512), F32),
            pltpu.VMEM((2, 4, 32, 512), F32),
            pltpu.VMEM((2, 4, 32, 512), F32),
            pltpu.VMEM((2, 2, 4, 16, 512), F32),
            pltpu.VMEM((256, 128), F32),
            pltpu.VMEM((32, 8, 128), F32),
            pltpu.VMEM((32, 256, 512), BF),
            pltpu.VMEM((32, 128, 512), BF),
            pltpu.VMEM((512, 256), F32),
            pltpu.VMEM((4, 256, 128), F32),
            pltpu.VMEM((32 * HS, 128), F32),
            pltpu.VMEM((64 * FS, 128), F32),
            pltpu.VMEM((4, 256, 128), F32),
            pltpu.VMEM((2, 256, 128), F32),
        ] + sems + [pltpu.SemaphoreType.DMA, pltpu.SemaphoreType.DMA],
        compiler_params=pltpu.CompilerParams(
            vmem_limit_bytes=56 << 20, collective_id=0, has_side_effects=True
        ),
        name="panel",
    )(rot, pot, coef, idx, counts, *consts)


def per_device(coefficients, rotation, potential, index_map, counts):
    coef = coefficients.reshape(256, 2, 4, 128).transpose(0, 2, 1, 3).reshape(2048, 128)
    return run(
        rotation.transpose(0, 2, 1), potential, coef, index_map.reshape(128, 128), counts
    )


def solution(mesh):
    torus = Mesh(mesh.devices.reshape(4, 4, 2, 4, 2), GA + BAND)
    return jax.shard_map(
        per_device,
        mesh=torus,
        in_specs=(P(BAND, None, GA), P(None, BAND, GA), P(None, GA), P(), P()),
        out_specs=P(BAND + GA, None, None, None),
        check_vma=False,
    )
```

```python
import math

import jax
import jax.numpy as jnp
import numpy as np
from jax import lax
from jax.experimental import pallas as pl
from jax.experimental.pallas import tpu as pltpu
from jax.sharding import Mesh
from jax.sharding import PartitionSpec as P

F32 = jnp.float32
BF = jnp.bfloat16
MESH = pl.DeviceIdType.MESH
GA = ("ga_0", "ga_1", "ga_2")
BAND = ("band_0", "band_1")
HS = 72
FS = 40


def split_np(a):
    a = np.asarray(a, np.float32)
    hi = a.astype(BF)
    lo = (a - hi.astype(np.float32)).astype(BF)
    return hi, lo


def stack3(a):
    hi, lo = split_np(a)
    return np.concatenate([hi, hi, lo], axis=1)


def tables():
    n = np.arange(32) - 16
    r = np.arange(64)
    ang = 2.0 * math.pi * ((r[:, None] * n[None, :]) % 64) / 64.0
    cos, sin = np.cos(ang), np.sin(ang)
    perm = np.array([(k % 8) * 4 + k // 8 for k in range(32)])
    s = 8.0 / 4096.0
    wz = np.zeros((2, 4, 32, 2, 4, 2, 64))
    for q in range(4):
        wz[0, q, :, 0, q, 0, :] = cos.T / 64
        wz[1, q, :, 0, q, 0, :] = -sin.T / 64
        wz[0, q, :, 0, q, 1, :] = sin.T / 64
        wz[1, q, :, 0, q, 1, :] = cos.T / 64
    wz[:, :, :, 1] = wz[:, :, :, 0] * (s * n * n)[None, None, :, None, None, None]
    wz_h, wz_l = split_np(wz.reshape(256, 1024))
    ty = stack3(np.concatenate([cos[:, perm], sin[:, perm]], axis=1) / 64)
    tx = stack3(np.concatenate([cos, sin], axis=1) / 64)
    fx = stack3(np.concatenate([cos.T, sin.T], axis=0))
    fy = stack3(np.concatenate([cos.T[perm], sin.T[perm]], axis=0))
    wf = np.zeros((4, 2, 64, 2, 4, 32))
    for q in range(4):
        wf[q, 0, :, 0, q, :] = cos
        wf[q, 1, :, 0, q, :] = sin
        wf[q, 1, :, 1, q, :] = cos
        wf[q, 0, :, 1, q, :] = -sin
    wf_h, wf_l = split_np(wf.reshape(512, 256))
    return [wz_h, wz_l, ty, tx, fx, fy, wf_h, wf_l]


def split(a):
    hi = a.astype(BF)
    return hi, (a - hi.astype(F32)).astype(BF)


def dot(a, b):
    return jnp.dot(a, b, preferred_element_type=F32)


def kernel(
    rot_in, pot_in, coef_in, idx_in, counts_in,
    wz_h_in, wz_l_in, ty_in, tx_in, fx_in, fy_in, wf_h_in, wf_l_in,
    out,
    rot, pot, coef, idx, counts, wz_h, wz_l, ty, tx, fx, fy, wf_h, wf_l,
    rg, vg, ch, cl, sb, sr, pb, rz, ab, vals, cols, rows, acc, ek, h, f, gz, o,
    l_sem, r_send, r_recv, v_send, v_recv, s_send, s_recv, z_send, z_recv,
    a_send, a_recv, w_send, w_recv,
):
    y, x, zh = lax.axis_index("ga_0"), lax.axis_index("ga_1"), lax.axis_index("ga_2")
    zl, core = lax.axis_index("band_0"), lax.axis_index("band_1")
    g = y * 8 + x * 2 + zh
    far = y * 8 + x * 2 + (1 - zh)
    half = pl.multiple_of(core * 32, 32)
    other = {"ga_2": 1 - zh}
    sibling = {"band_1": 1 - core}

    local = [
        pltpu.make_async_copy(a, b, l_sem.at[n])
        for n, (a, b) in enumerate([
            (rot_in.at[:, :, 0:128], rot.at[0]), (coef_in, coef), (pot_in, pot), (idx_in, idx),
            (counts_in, counts), (wz_h_in, wz_h), (wz_l_in, wz_l), (ty_in, ty),
            (tx_in, tx), (fx_in, fx), (fy_in, fy), (wf_h_in, wf_h), (wf_l_in, wf_l),
            (rot_in.at[:, :, 128:256], rot.at[1]),
        ])
    ]
    local[0].start()
    local[13].start()

    def mate(i):
        a, b = i // 4, i % 4
        yy = (y + (a ^ (a >> 1))) % 4
        xx = (x + (b ^ (b >> 1))) % 4
        return yy * 4 + xx, {"ga_0": yy, "ga_1": xx}

    barrier = pltpu.get_barrier_semaphore()

    def greet(i, _):
        pl.semaphore_signal(barrier, inc=1, device_id=mate(16 - i)[1], device_id_type=MESH)
        return 0

    def hop(i, _):
        p = (zl * 2 + core + i) % 8
        to = {"band_0": p // 2, "band_1": p % 2}
        pl.semaphore_signal(barrier, inc=1, device_id=to, device_id_type=MESH)
        return 0

    pl.semaphore_signal(barrier, inc=1, device_id=other, device_id_type=MESH)
    lax.fori_loop(1, 16, greet, 0)
    lax.fori_loop(1, 8, hop, 0)

    for n in range(1, 13):
        local[n].start()
    local[0].wait()
    local[13].wait()
    for t in range(2):
        for s in range(2):
            for r in range(2):
                rg[g, s, r * 4 : r * 4 + 4, t * 128 : t * 128 + 128] = rot[
                    t, r, pl.ds(s, 4, stride=2), :
                ]
    local[2].wait()
    vg[g, pl.ds(half, 32), :] = pot[pl.ds(half, 32), :]
    pl.semaphore_wait(barrier, 23)

    def send(src, dst, send_sem, recv_sem, to):
        return pltpu.make_async_remote_copy(
            src_ref=src, dst_ref=dst, send_sem=send_sem, recv_sem=recv_sem,
            device_id=to, device_id_type=MESH,
        )

    def rot_copy(block, i, to):
        return send(rg.at[block], rg.at[block], r_send.at[i], r_recv.at[block], to)

    def pot_copy(block, i, to):
        piece = vg.at[block, pl.ds(half, 32)]
        return send(piece, piece, v_send.at[i], v_recv.at[block], to)

    def each(lo, copy, hi=16):
        def step(i, _):
            copy(i).start()
            return 0

        lax.fori_loop(lo, hi, step, 0)

    rot_copy(g, 0, other).start()
    each(1, lambda i: rot_copy(g, i, mate(i)[1]))
    pot_copy(g, 0, other).start()

    local[1].wait()
    for c in range(2):
        for t in range(4):
            hi, lo = split(coef[pl.ds(t * 2 + c, 256, stride=8), :])
            ch[c * 256 : c * 256 + 256, t * 128 : t * 128 + 128] = hi
            cl[c * 256 : c * 256 + 256, t * 128 : t * 128 + 128] = lo

    local[3].wait()
    local[4].wait()
    rows128 = lax.broadcasted_iota(jnp.int32, (128, 512), 0)
    rows256 = lax.broadcasted_iota(jnp.int32, (256, 512), 0)
    slot = lax.broadcasted_iota(jnp.int32, (1, 512), 1)

    def one_hot(k, _):
        cell = jnp.concatenate([idx[pl.ds(k * 4 + t, 1), :] for t in range(4)], axis=1)
        wx = ((cell >> 12) + 16) & 63
        wy = ((cell >> 6) + 16) & 63
        wz = (cell + 16) & 63
        at_lane = (wx & 7) * 32 + wz
        at_row = (wx >> 3) * 32 + (wy & 3) * 8 + ((wy >> 2) & 7)
        at_row = jnp.where(slot < counts[k], at_row, -1)
        cols[k] = jnp.where(rows256 == at_lane, 1.0, 0.0).astype(BF)
        rows[k] = jnp.where(rows128 == at_row, 1.0, 0.0).astype(BF)
        return 0

    acc[...] = jnp.zeros_like(acc)
    sub = lax.broadcasted_iota(jnp.int32, (8, 256), 0)
    flip = jnp.where(sub < 4, -1.0, 1.0).astype(F32)

    def row_of(n):
        return (y + (n ^ (n >> 1))) % 4

    def plane_of(q):
        return zh if q == 0 else 1 - zh

    def pair_copy(q, d):
        return send(sb.at[q, d], sr.at[q, d], s_send.at[q * 4 + d], s_recv.at[q * 4 + d], sibling)

    def chip_copy(q, d, away, src):
        to = {"band_0": d, **sibling}
        if away:
            to["ga_2"] = 1 - zh
        return send(
            pb.at[q, d, pl.ds(away * 16, 16)], rz.at[q, away, src],
            z_send.at[q * 8 + d * 2 + away], z_recv.at[q * 8 + src * 2 + away], to,
        )

    def mix(q, n):
        d = row_of(n)

        def rot_wait(i, _):
            p, to = mate(i)
            rot_copy(p * 2 + plane_of(q), 0, to).wait_recv()
            return 0

        lax.fori_loop(max(1, n * 4), n * 4 + 4, rot_wait, 0)
        left, right = [], []
        for parity in (1 - core, core):
            for t in (zh, 1 - zh):
                for xb in range(2):
                    block = rg[d * 8 + (parity * 2 + xb) * 2 + plane_of(q), t]
                    left.append(block)
                    right.append(flip * pltpu.roll(block, 4, 0))
        lh, ll = split(jnp.concatenate([jnp.concatenate(left, 0), jnp.concatenate(right, 0)], 1))
        high = dot(jnp.concatenate([lh, ll], axis=0), ch[...])
        both = high[0:64] + high[64:128] + dot(lh, cl[...])
        sb[q, d] = both[0:32]
        pb[q, d] = both[32:64]
        pair_copy(q, d).start()

    def settle(q, n):
        d = row_of(n)
        pair_copy(q, d).wait_recv()
        pb[q, d] = pb[q, d] + sr[q, d]
        chip_copy(q, d, 1, zl).start()
        chip_copy(q, d, 0, zl).start()

    def band_copy(q, i):
        away, xb, xx = 1 - i // 8, (i // 4) % 2, (x + 3 - i % 4) % 4
        source = plane_of(away)
        yy = xb * 2 + plane_of(q ^ away)
        slot16 = yy * 4 + xx
        src = ab.at[pl.ds(pl.multiple_of(away * 128 + slot16 * 8, 8), 8)]
        block = (y * 4 + x) * 2 + source
        to = {"ga_0": yy, "ga_1": xx, **sibling}
        return send(
            src, vals.at[block], a_send.at[away * 16 + slot16], a_recv.at[block], to
        )

    def finish(q):
        for away in (1, 0):
            total = None
            for src in range(4):
                chip_copy(q, zl, away, src).wait_recv()
                part = rz[q, away, src]
                total = part if total is None else total + part
            for xb in range(2):
                for c in range(2):
                    for t in range(4):
                        start = away * 128 + (xb * 2 + plane_of(q ^ away)) * 32 + c * 4 + t
                        at = xb * 8 + c * 4
                        ab[pl.ds(start, 4, stride=8), :] = total[at : at + 4, t * 128 : t * 128 + 128]
            for i in range(8):
                band_copy(q, i + 8 * (1 - away)).start()

    lax.fori_loop(0, 32, one_hot, 0)
    mix(0, 0)
    rot_copy(far, 16, other).wait_recv()
    each(1, lambda i: rot_copy(far, 16 + i, mate(i)[1]))
    mix(0, 1)
    settle(0, 0)
    mix(0, 2)
    settle(0, 1)
    mix(0, 3)
    settle(0, 2)
    mix(1, 0)
    settle(0, 3)
    each(1, lambda i: pot_copy(g, i, mate(i)[1]))
    mix(1, 1)
    settle(1, 0)
    pot_copy(far, 16, other).wait_recv()
    each(1, lambda i: pot_copy(far, 16 + i, mate(i)[1]))
    mix(1, 2)
    settle(1, 1)
    mix(1, 3)
    settle(1, 2)
    settle(1, 3)
    finish(0)
    def pot_wait(i, _):
        p, to = mate(i)
        pot_copy(p * 2, 0, to).wait_recv()
        pot_copy(p * 2 + 1, 0, to).wait_recv()
        return 0

    lax.fori_loop(1, 16, pot_wait, 0)
    side = vg.at[:, pl.ds(half, 32)]
    swap = send(side, side, w_send, w_recv, sibling)
    swap.start()
    finish(1)
    def place(i, plane):
        left, right = [], []
        for b in range(4):
            k = mate(i * 4 + b)[0] * 2 + plane
            send(ab.at[pl.ds(0, 8)], vals.at[k], a_send.at[0], a_recv.at[k], sibling).wait_recv()

        for b in range(4):
            k = mate(i * 4 + b)[0] * 2 + plane
            hit = rows[k]
            parts = []
            for c in range(2):
                v = jnp.concatenate([vals[k, pl.ds(c * 4 + t, 1), :] for t in range(4)], axis=1)
                high = v.astype(BF).astype(F32)
                for part in (high, v - high):
                    wide = jnp.broadcast_to(part, (16, 512)).astype(BF)
                    parts.append(hit * jnp.concatenate([wide] * 8, axis=0))
            left.append(jnp.concatenate(parts, axis=0))
            right.append(cols[k])
        return lax.dot_general(
            jnp.concatenate(left, axis=1), jnp.concatenate(right, axis=1),
            (((1,), (1,)), ((), ())), preferred_element_type=F32,
        )

    soon = y % 2
    def place_step(i, _):
        acc[...] += place(i % 4, jnp.where(i < 4, soon, 1 - soon))
        return 0

    lax.fori_loop(0, 8, place_step, 0)

    for copy in local[5:13]:
        copy.wait()
    lane = lax.broadcasted_iota(jnp.int32, (1, 128), 1)
    turn = jnp.where(lane < 64, -1.0, 1.0).astype(F32)
    re = acc[0:128, :] + acc[128:256, :]
    im = acc[256:384, :] + acc[384:512, :]
    nrow = lax.broadcasted_iota(jnp.int32, (32, 128), 0)
    ny = ((nrow & 7) * 4 + (nrow >> 3) - 16).astype(F32)
    ksq = (8.0 / 4096.0) * ny * ny
    e = []
    for t in range(2):
        d = jnp.concatenate([re[:, t * 128 : t * 128 + 128], im[:, t * 128 : t * 128 + 128]], axis=1)
        dh, dl = split(d)
        e.append(dot(dh, wz_h[...]) + dot(dl, wz_h[...]) + dot(dh, wz_l[...]))

    def column(i):
        xh, t, q = i // 8, (i // 4) % 2, i % 4
        tile = e[t][xh * 32 : xh * 32 + 32, q * 128 : q * 128 + 128]
        bent = e[t][xh * 32 : xh * 32 + 32, 512 + q * 128 : 512 + q * 128 + 128]
        kin = (ksq + (8.0 / 4096.0) * (i - 16) ** 2) * tile + bent
        for j in range(4):
            ek[j, i * 8 : i * 8 + 8, :] = kin[j * 8 : j * 8 + 8, :]
        return jnp.concatenate([tile, turn * pltpu.roll(tile, 64, 1)], axis=0)

    for i in range(0, 32, 2):
        dh, dl = split(jnp.concatenate([column(i), column(i + 1)], axis=1))
        d = dot(ty[...], jnp.concatenate([dh, dl, dh], axis=0))
        h[i * HS : i * HS + 64, :] = d[:, 0:128]
        h[(i + 1) * HS : (i + 1) * HS + 64, :] = d[:, 128:256]

    swap.wait()

    def plane(i, _):
        both = []
        for q in range(2):
            tile = h[pl.ds(i * 2 + q, 32, stride=HS), :]
            both.append(jnp.concatenate([tile, turn * pltpu.roll(tile, 64, 1)], axis=0))
        dh, dl = split(jnp.concatenate(both, axis=1))
        real = dot(tx[...], jnp.concatenate([dh, dl, dh], axis=0))
        v = vg[i]
        vr = pltpu.roll(v, 64, 1)
        low = lane < 64
        vv = jnp.concatenate([jnp.where(low, v, vr), jnp.where(low, vr, v)], axis=1)
        dh, dl = split(real * vv)
        pq = dot(fx[...], jnp.concatenate([dh, dl, dh], axis=0))
        for q in range(2):
            pp = pq[0:32, q * 128 : q * 128 + 128]
            qq = pq[32:64, q * 128 : q * 128 + 128]
            start = pl.multiple_of((i * 2 + q) * FS, 8)
            f[pl.ds(start, 32), :] = pp - turn * pltpu.roll(qq, 64, 1)
        return 0

    lax.fori_loop(0, 32, plane, 0, unroll=32)

    def line(i, _):
        d = jnp.concatenate([f[pl.ds(i * 2 + q, 64, stride=FS), :] for q in range(2)], axis=1)
        dh, dl = split(d)
        pq = dot(fy[...], jnp.concatenate([dh, dl, dh], axis=0))
        for q in range(2):
            pp = pq[0:32, q * 128 : q * 128 + 128]
            qq = pq[32:64, q * 128 : q * 128 + 128]
            yy = pp - turn * pltpu.roll(qq, 64, 1)
            start = pl.multiple_of((i * 2 + q) * 8, 8)
            for j in range(4):
                gz[j, pl.ds(start, 8), :] = yy[j * 8 : j * 8 + 8, :] + ek[j, pl.ds(start, 8), :]
        return 0

    lax.fori_loop(0, 16, line, 0, unroll=16)

    dh, dl = split(jnp.concatenate([gz[j] for j in range(4)], axis=1))
    z = dot(dh, wf_h[...]) + dot(dl, wf_h[...]) + dot(dh, wf_l[...])
    for c in range(2):
        o[c] = z[:, c * 128 : c * 128 + 128]
        for b in range(8):
            out[0, c, :, b * 128 : b * 128 + 128] = o[c, pl.ds(b, 32, stride=8), :]

    rot_copy(g, 0, other).wait_send()
    pot_copy(g, 0, other).wait_send()

    def sent(i, _):
        to = mate(i)[1]
        rot_copy(g, i, to).wait_send()
        rot_copy(far, 16 + i, to).wait_send()
        pot_copy(g, i, to).wait_send()
        pot_copy(far, 16 + i, to).wait_send()
        return 0

    lax.fori_loop(1, 16, sent, 0)
    for q in range(2):
        for d in range(4):
            pair_copy(q, d).wait_send()
            chip_copy(q, d, 1, 0).wait_send()
            chip_copy(q, d, 0, 0).wait_send()
        for i in range(16):
            band_copy(q, i).wait_send()


def run(rot, pot, coef, idx, counts):
    consts = [jnp.asarray(c) for c in tables()]
    hbm = pl.BlockSpec(memory_space=pltpu.HBM)
    sems = [pltpu.SemaphoreType.DMA((n,)) for n in (14, 32, 32, 32, 32, 8, 8, 16, 16, 32, 32)]
    return pl.pallas_call(
        kernel,
        out_shape=jax.ShapeDtypeStruct((1, 2, 32, 1024), F32),
        in_specs=[hbm] * 13,
        out_specs=pl.BlockSpec(memory_space=pltpu.VMEM),
        scratch_shapes=[
            pltpu.VMEM((2, 2, 8, 128), F32),
            pltpu.VMEM((64, 128), F32),
            pltpu.VMEM((2048, 128), F32),
            pltpu.VMEM((128, 128), jnp.int32),
            pltpu.SMEM((32,), jnp.int32),
        ] + [pltpu.VMEM(c.shape, c.dtype) for c in consts] + [
            pltpu.VMEM((32, 2, 8, 256), F32),
            pltpu.VMEM((32, 64, 128), F32),
            pltpu.VMEM((512, 512), BF),
            pltpu.VMEM((512, 512), BF),
            pltpu.VMEM((2, 4, 32, 512), F32),
            pltpu.VMEM((2, 4, 32, 512), F32),
            pltpu.VMEM((2, 4, 32, 512), F32),
            pltpu.VMEM((2, 2, 4, 16, 512), F32),
            pltpu.VMEM((256, 128), F32),
            pltpu.VMEM((32, 8, 128), F32),
            pltpu.VMEM((32, 256, 512), BF),
            pltpu.VMEM((32, 128, 512), BF),
            pltpu.VMEM((512, 256), F32),
            pltpu.VMEM((4, 256, 128), F32),
            pltpu.VMEM((32 * HS, 128), F32),
            pltpu.VMEM((64 * FS, 128), F32),
            pltpu.VMEM((4, 256, 128), F32),
            pltpu.VMEM((2, 256, 128), F32),
        ] + sems + [pltpu.SemaphoreType.DMA, pltpu.SemaphoreType.DMA],
        compiler_params=pltpu.CompilerParams(
            vmem_limit_bytes=56 << 20, collective_id=0, has_side_effects=True
        ),
        name="panel",
    )(rot, pot, coef, idx, counts, *consts)


def per_device(coefficients, rotation, potential, index_map, counts):
    coef = coefficients.reshape(256, 2, 4, 128).transpose(0, 2, 1, 3).reshape(2048, 128)
    return run(
        rotation.transpose(0, 2, 1), potential, coef, index_map.reshape(128, 128), counts
    )


def solution(mesh):
    torus = Mesh(mesh.devices.reshape(4, 4, 2, 4, 2), GA + BAND)
    return jax.shard_map(
        per_device,
        mesh=torus,
        in_specs=(P(BAND, None, GA), P(None, BAND, GA), P(None, GA), P(), P()),
        out_specs=P(BAND + GA, None, None, None),
        check_vma=False,
    )
```

```python
import math

import jax
import jax.numpy as jnp
import numpy as np
from jax import lax
from jax.experimental import pallas as pl
from jax.experimental.pallas import tpu as pltpu
from jax.sharding import Mesh
from jax.sharding import PartitionSpec as P

F32 = jnp.float32
BF = jnp.bfloat16
MESH = pl.DeviceIdType.MESH
GA = ("ga_0", "ga_1", "ga_2")
BAND = ("band_0", "band_1")
HS = 72
FS = 40


def split_np(a):
    a = np.asarray(a, np.float32)
    hi = a.astype(BF)
    lo = (a - hi.astype(np.float32)).astype(BF)
    return hi, lo


def stack3(a):
    hi, lo = split_np(a)
    return np.concatenate([hi, hi, lo], axis=1)


def tables():
    n = np.arange(32) - 16
    r = np.arange(64)
    ang = 2.0 * math.pi * ((r[:, None] * n[None, :]) % 64) / 64.0
    cos, sin = np.cos(ang), np.sin(ang)
    perm = np.array([(k % 8) * 4 + k // 8 for k in range(32)])
    wz = np.zeros((2, 4, 32, 4, 2, 64))
    for q in range(4):
        wz[0, q, :, q, 0, :] = cos.T / 64
        wz[1, q, :, q, 0, :] = -sin.T / 64
        wz[0, q, :, q, 1, :] = sin.T / 64
        wz[1, q, :, q, 1, :] = cos.T / 64
    wz_h, wz_l = split_np(wz.reshape(256, 512))
    ty = stack3(np.concatenate([cos[:, perm], sin[:, perm]], axis=1) / 64)
    tx = stack3(np.concatenate([cos, sin], axis=1) / 64)
    fx = stack3(np.concatenate([cos.T, sin.T], axis=0))
    fy = stack3(np.concatenate([cos.T[perm], sin.T[perm]], axis=0))
    wf = np.zeros((4, 2, 64, 2, 4, 32))
    for q in range(4):
        wf[q, 0, :, 0, q, :] = cos
        wf[q, 1, :, 0, q, :] = sin
        wf[q, 1, :, 1, q, :] = cos
        wf[q, 0, :, 1, q, :] = -sin
    wf_h, wf_l = split_np(wf.reshape(512, 256))
    return [wz_h, wz_l, ty, tx, fx, fy, wf_h, wf_l]


def split(a):
    hi = a.astype(BF)
    return hi, (a - hi.astype(F32)).astype(BF)


def dot(a, b):
    return jnp.dot(a, b, preferred_element_type=F32)


def kernel(
    rot_in, pot_in, coef_in, idx_in, counts_in,
    wz_h_in, wz_l_in, ty_in, tx_in, fx_in, fy_in, wf_h_in, wf_l_in,
    out,
    rot, pot, coef, idx, counts, wz_h, wz_l, ty, tx, fx, fy, wf_h, wf_l,
    rg, vg, ch, cl, sb, sr, pb, rz, ab, vals, cols, rows, acc, ek, h, f, gz, o, res,
    l_sem, r_send, r_recv, v_send, v_recv, s_send, s_recv, z_send, z_recv,
    a_send, a_recv, w_send, w_recv,
):
    y, x, zh = lax.axis_index("ga_0"), lax.axis_index("ga_1"), lax.axis_index("ga_2")
    zl, core = lax.axis_index("band_0"), lax.axis_index("band_1")
    g = y * 8 + x * 2 + zh
    far = y * 8 + x * 2 + (1 - zh)
    half = pl.multiple_of(core * 32, 32)
    other = {"ga_2": 1 - zh}
    sibling = {"band_1": 1 - core}

    local = [
        pltpu.make_async_copy(a, b, l_sem.at[n])
        for n, (a, b) in enumerate([
            (rot_in.at[:, :, 0:128], rot.at[0]), (coef_in, coef), (pot_in, pot), (idx_in, idx),
            (counts_in, counts), (wz_h_in, wz_h), (wz_l_in, wz_l), (ty_in, ty),
            (tx_in, tx), (fx_in, fx), (fy_in, fy), (wf_h_in, wf_h), (wf_l_in, wf_l),
            (rot_in.at[:, :, 128:256], rot.at[1]),
        ])
    ]
    local[0].start()
    local[13].start()

    def mate(i):
        a, b = i // 4, i % 4
        yy = (y + (a ^ (a >> 1))) % 4
        xx = (x + (b ^ (b >> 1))) % 4
        return yy * 4 + xx, {"ga_0": yy, "ga_1": xx}

    barrier = pltpu.get_barrier_semaphore()

    def greet(i, _):
        pl.semaphore_signal(barrier, inc=1, device_id=mate(16 - i)[1], device_id_type=MESH)
        return 0

    def hop(i, _):
        p = (zl * 2 + core + i) % 8
        to = {"band_0": p // 2, "band_1": p % 2}
        pl.semaphore_signal(barrier, inc=1, device_id=to, device_id_type=MESH)
        return 0

    pl.semaphore_signal(barrier, inc=1, device_id=other, device_id_type=MESH)
    lax.fori_loop(1, 16, greet, 0)
    lax.fori_loop(1, 8, hop, 0)

    for n in range(1, 13):
        local[n].start()
    local[0].wait()
    local[13].wait()
    for t in range(2):
        for s in range(2):
            for r in range(2):
                rg[g, s, r * 4 : r * 4 + 4, t * 128 : t * 128 + 128] = rot[
                    t, r, pl.ds(s, 4, stride=2), :
                ]
    local[2].wait()
    vg[g, pl.ds(half, 32), :] = pot[pl.ds(half, 32), :]
    pl.semaphore_wait(barrier, 23)

    def send(src, dst, send_sem, recv_sem, to):
        return pltpu.make_async_remote_copy(
            src_ref=src, dst_ref=dst, send_sem=send_sem, recv_sem=recv_sem,
            device_id=to, device_id_type=MESH,
        )

    def rot_copy(block, i, to):
        return send(rg.at[block], rg.at[block], r_send.at[i], r_recv.at[block], to)

    def pot_copy(block, i, to):
        piece = vg.at[block, pl.ds(half, 32)]
        return send(piece, piece, v_send.at[i], v_recv.at[block], to)

    def each(lo, copy, hi=16):
        def step(i, _):
            copy(i).start()
            return 0

        lax.fori_loop(lo, hi, step, 0)

    rot_copy(g, 0, other).start()
    each(1, lambda i: rot_copy(g, i, mate(i)[1]))
    pot_copy(g, 0, other).start()

    local[1].wait()
    for c in range(2):
        for t in range(4):
            hi, lo = split(coef[pl.ds(t * 2 + c, 256, stride=8), :])
            ch[c * 256 : c * 256 + 256, t * 128 : t * 128 + 128] = hi
            cl[c * 256 : c * 256 + 256, t * 128 : t * 128 + 128] = lo

    local[3].wait()
    local[4].wait()
    rows128 = lax.broadcasted_iota(jnp.int32, (128, 512), 0)
    rows256 = lax.broadcasted_iota(jnp.int32, (256, 512), 0)
    slot = lax.broadcasted_iota(jnp.int32, (1, 512), 1)

    def one_hot(k, _):
        cell = jnp.concatenate([idx[pl.ds(k * 4 + t, 1), :] for t in range(4)], axis=1)
        wx = ((cell >> 12) + 16) & 63
        wy = ((cell >> 6) + 16) & 63
        wz = (cell + 16) & 63
        at_lane = (wx & 7) * 32 + wz
        at_row = (wx >> 3) * 32 + (wy & 3) * 8 + ((wy >> 2) & 7)
        at_row = jnp.where(slot < counts[k], at_row, -1)
        cols[k] = jnp.where(rows256 == at_lane, 1.0, 0.0).astype(BF)
        rows[k] = jnp.where(rows128 == at_row, 1.0, 0.0).astype(BF)
        return 0

    acc[...] = jnp.zeros_like(acc)
    sub = lax.broadcasted_iota(jnp.int32, (8, 256), 0)
    flip = jnp.where(sub < 4, -1.0, 1.0).astype(F32)

    def row_of(n):
        return (y + (n ^ (n >> 1))) % 4

    def plane_of(q):
        return zh if q == 0 else 1 - zh

    def pair_copy(q, d):
        return send(sb.at[q, d], sr.at[q, d], s_send.at[q * 4 + d], s_recv.at[q * 4 + d], sibling)

    def chip_copy(q, d, away, src):
        to = {"band_0": d, **sibling}
        if away:
            to["ga_2"] = 1 - zh
        return send(
            pb.at[q, d, pl.ds(away * 16, 16)], rz.at[q, away, src],
            z_send.at[q * 8 + d * 2 + away], z_recv.at[q * 8 + src * 2 + away], to,
        )

    def mix(q, n):
        d = row_of(n)

        def rot_wait(i, _):
            p, to = mate(i)
            rot_copy(p * 2 + plane_of(q), 0, to).wait_recv()
            return 0

        lax.fori_loop(max(1, n * 4), n * 4 + 4, rot_wait, 0)
        left, right = [], []
        for parity in (1 - core, core):
            for t in (zh, 1 - zh):
                for xb in range(2):
                    block = rg[d * 8 + (parity * 2 + xb) * 2 + plane_of(q), t]
                    left.append(block)
                    right.append(flip * pltpu.roll(block, 4, 0))
        lh, ll = split(jnp.concatenate([jnp.concatenate(left, 0), jnp.concatenate(right, 0)], 1))
        high = dot(jnp.concatenate([lh, ll], axis=0), ch[...])
        both = high[0:64] + high[64:128] + dot(lh, cl[...])
        sb[q, d] = both[0:32]
        pb[q, d] = both[32:64]
        pair_copy(q, d).start()

    def settle(q, n):
        d = row_of(n)
        pair_copy(q, d).wait_recv()
        pb[q, d] = pb[q, d] + sr[q, d]
        chip_copy(q, d, 1, zl).start()
        chip_copy(q, d, 0, zl).start()

    def band_copy(q, i):
        away, xb, xx = 1 - i // 8, (i // 4) % 2, (x + 3 - i % 4) % 4
        source = plane_of(away)
        yy = xb * 2 + plane_of(q ^ away)
        slot16 = yy * 4 + xx
        src = ab.at[pl.ds(pl.multiple_of(away * 128 + slot16 * 8, 8), 8)]
        block = (y * 4 + x) * 2 + source
        to = {"ga_0": yy, "ga_1": xx, **sibling}
        return send(
            src, vals.at[block], a_send.at[away * 16 + slot16], a_recv.at[block], to
        )

    def finish(q):
        for away in (1, 0):
            total = None
            for src in range(4):
                chip_copy(q, zl, away, src).wait_recv()
                part = rz[q, away, src]
                total = part if total is None else total + part
            for xb in range(2):
                for c in range(2):
                    for t in range(4):
                        start = away * 128 + (xb * 2 + plane_of(q ^ away)) * 32 + c * 4 + t
                        at = xb * 8 + c * 4
                        ab[pl.ds(start, 4, stride=8), :] = total[at : at + 4, t * 128 : t * 128 + 128]
            for i in range(8):
                band_copy(q, i + 8 * (1 - away)).start()

    lax.fori_loop(0, 32, one_hot, 0)
    mix(0, 0)
    rot_copy(far, 16, other).wait_recv()
    each(1, lambda i: rot_copy(far, 16 + i, mate(i)[1]))
    mix(0, 1)
    settle(0, 0)
    mix(0, 2)
    settle(0, 1)
    mix(0, 3)
    settle(0, 2)
    mix(1, 0)
    settle(0, 3)
    each(1, lambda i: pot_copy(g, i, mate(i)[1]))
    mix(1, 1)
    settle(1, 0)
    pot_copy(far, 16, other).wait_recv()
    each(1, lambda i: pot_copy(far, 16 + i, mate(i)[1]))
    mix(1, 2)
    settle(1, 1)
    mix(1, 3)
    settle(1, 2)
    settle(1, 3)
    finish(0)
    def pot_wait(i, _):
        p, to = mate(i)
        pot_copy(p * 2, 0, to).wait_recv()
        pot_copy(p * 2 + 1, 0, to).wait_recv()
        return 0

    lax.fori_loop(1, 16, pot_wait, 0)
    side = vg.at[:, pl.ds(half, 32)]
    swap = send(side, side, w_send, w_recv, sibling)
    swap.start()
    finish(1)
    def place(i, plane):
        left, right = [], []
        for b in range(4):
            k = mate(i * 4 + b)[0] * 2 + plane
            send(ab.at[pl.ds(0, 8)], vals.at[k], a_send.at[0], a_recv.at[k], sibling).wait_recv()

        for b in range(4):
            k = mate(i * 4 + b)[0] * 2 + plane
            hit = rows[k]
            parts = []
            for c in range(2):
                v = jnp.concatenate([vals[k, pl.ds(c * 4 + t, 1), :] for t in range(4)], axis=1)
                high = v.astype(BF).astype(F32)
                for part in (high, v - high):
                    wide = jnp.broadcast_to(part, (16, 512)).astype(BF)
                    parts.append(hit * jnp.concatenate([wide] * 8, axis=0))
            left.append(jnp.concatenate(parts, axis=0))
            right.append(cols[k])
        return lax.dot_general(
            jnp.concatenate(left, axis=1), jnp.concatenate(right, axis=1),
            (((1,), (1,)), ((), ())), preferred_element_type=F32,
        )

    soon = y % 2
    def place_step(i, _):
        acc[...] += place(i % 4, jnp.where(i < 4, soon, 1 - soon))
        return 0

    lax.fori_loop(0, 8, place_step, 0)

    for copy in local[5:13]:
        copy.wait()
    lane = lax.broadcasted_iota(jnp.int32, (1, 128), 1)
    turn = jnp.where(lane < 64, -1.0, 1.0).astype(F32)
    re = acc[0:128, :] + acc[128:256, :]
    im = acc[256:384, :] + acc[384:512, :]
    both = jnp.concatenate([re, im], axis=1)
    d = jnp.concatenate(
        [
            jnp.concatenate([v[:, t * 128 : t * 128 + 128] for v in (re, im)], axis=1)
            for t in range(2)
        ],
        axis=0,
    )
    dh, dl = split(d)
    e = dot(dh, wz_h[...]) + dot(dl, wz_h[...]) + dot(dh, wz_l[...])

    lane8 = lax.broadcasted_iota(jnp.int32, (8, 128), 1)
    high = lax.broadcasted_iota(jnp.int32, (8, 128), 0)
    ny = (high * 4 + (lane8 >> 5) - 16).astype(F32)
    nz = ((lane8 & 31) - 16).astype(F32)
    kyz = (8.0 / 4096.0) * (ny * ny + nz * nz)
    quarter = lax.broadcasted_iota(jnp.int32, (1, 128), 1) >> 5
    lines = [
        jnp.concatenate(
            [
                both[xh * 32 + j * 8 : xh * 32 + j * 8 + 8, ct * 128 : ct * 128 + 128]
                for ct in range(4)
                for xh in range(4)
            ],
            axis=0,
        )
        for j in range(4)
    ]
    for q in range(4):
        turned = [
            lines[j] if j == q else pltpu.roll(lines[j], ((j - q) * 32) % 128, 1) for j in range(4)
        ]
        mixed = jnp.where(
            quarter < 2,
            jnp.where(quarter == 0, turned[0], turned[1]),
            jnp.where(quarter == 2, turned[2], turned[3]),
        )
        for ct in range(4):
            for xh in range(4):
                i = xh * 8 + (ct % 2) * 4 + q
                kin = kyz + (8.0 / 4096.0) * (i - 16) ** 2
                at = (ct * 4 + xh) * 8
                ek[ct // 2, i * 8 : i * 8 + 8, :] = kin * mixed[at : at + 8, :]

    def column(i):
        xh, t, q = i // 8, (i // 4) % 2, i % 4
        at = t * 128 + xh * 32
        tile = e[at : at + 32, q * 128 : q * 128 + 128]
        return jnp.concatenate([tile, turn * pltpu.roll(tile, 64, 1)], axis=0)

    for i in range(0, 32, 2):
        dh, dl = split(jnp.concatenate([column(i), column(i + 1)], axis=1))
        d = dot(ty[...], jnp.concatenate([dh, dl, dh], axis=0))
        h[i * HS : i * HS + 64, :] = d[:, 0:128]
        h[(i + 1) * HS : (i + 1) * HS + 64, :] = d[:, 128:256]

    swap.wait()

    def plane(i, _):
        both = []
        for q in range(2):
            tile = h[pl.ds(i * 2 + q, 32, stride=HS), :]
            both.append(jnp.concatenate([tile, turn * pltpu.roll(tile, 64, 1)], axis=0))
        dh, dl = split(jnp.concatenate(both, axis=1))
        real = dot(tx[...], jnp.concatenate([dh, dl, dh], axis=0))
        v = vg[i]
        vr = pltpu.roll(v, 64, 1)
        low = lane < 64
        vv = jnp.concatenate([jnp.where(low, v, vr), jnp.where(low, vr, v)], axis=1)
        dh, dl = split(real * vv)
        pq = dot(fx[...], jnp.concatenate([dh, dl, dh], axis=0))
        for q in range(2):
            pp = pq[0:32, q * 128 : q * 128 + 128]
            qq = pq[32:64, q * 128 : q * 128 + 128]
            start = pl.multiple_of((i * 2 + q) * FS, 8)
            f[pl.ds(start, 32), :] = pp - turn * pltpu.roll(qq, 64, 1)
        return 0

    lax.fori_loop(0, 32, plane, 0, unroll=32)

    def line(i, _):
        d = jnp.concatenate([f[pl.ds(i * 2 + q, 64, stride=FS), :] for q in range(2)], axis=1)
        dh, dl = split(d)
        pq = dot(fy[...], jnp.concatenate([dh, dl, dh], axis=0))
        for q in range(2):
            pp = pq[0:32, q * 128 : q * 128 + 128]
            qq = pq[32:64, q * 128 : q * 128 + 128]
            yy = pp - turn * pltpu.roll(qq, 64, 1)
            start = pl.multiple_of((i * 2 + q) * 8, 8)
            for j in range(4):
                gz[j, pl.ds(start, 8), :] = yy[j * 8 : j * 8 + 8, :]
        return 0

    lax.fori_loop(0, 16, line, 0, unroll=16)

    dh, dl = split(jnp.concatenate([gz[j] for j in range(4)], axis=1))
    z = dot(dh, wf_h[...]) + dot(dl, wf_h[...]) + dot(dh, wf_l[...])
    def result(c):
        return pltpu.make_async_copy(res.at[c], out.at[0, c], l_sem.at[c])

    for c in range(2):
        o[c] = z[:, c * 128 : c * 128 + 128] + ek[c]
        for b in range(8):
            res[c, :, b * 128 : b * 128 + 128] = o[c, pl.ds(b, 32, stride=8), :]
        result(c).start()

    rot_copy(g, 0, other).wait_send()
    pot_copy(g, 0, other).wait_send()

    def sent(i, _):
        to = mate(i)[1]
        rot_copy(g, i, to).wait_send()
        rot_copy(far, 16 + i, to).wait_send()
        pot_copy(g, i, to).wait_send()
        pot_copy(far, 16 + i, to).wait_send()
        return 0

    lax.fori_loop(1, 16, sent, 0)
    for q in range(2):
        for d in range(4):
            pair_copy(q, d).wait_send()
            chip_copy(q, d, 1, 0).wait_send()
            chip_copy(q, d, 0, 0).wait_send()
        for i in range(16):
            band_copy(q, i).wait_send()
    for c in range(2):
        result(c).wait()


def run(rot, pot, coef, idx, counts):
    consts = [jnp.asarray(c) for c in tables()]
    hbm = pl.BlockSpec(memory_space=pltpu.HBM)
    sems = [pltpu.SemaphoreType.DMA((n,)) for n in (14, 32, 32, 32, 32, 8, 8, 16, 16, 32, 32)]
    return pl.pallas_call(
        kernel,
        out_shape=jax.ShapeDtypeStruct((1, 2, 32, 1024), F32),
        in_specs=[hbm] * 13,
        out_specs=hbm,
        scratch_shapes=[
            pltpu.VMEM((2, 2, 8, 128), F32),
            pltpu.VMEM((64, 128), F32),
            pltpu.VMEM((2048, 128), F32),
            pltpu.VMEM((128, 128), jnp.int32),
            pltpu.SMEM((32,), jnp.int32),
        ] + [pltpu.VMEM(c.shape, c.dtype) for c in consts] + [
            pltpu.VMEM((32, 2, 8, 256), F32),
            pltpu.VMEM((32, 64, 128), F32),
            pltpu.VMEM((512, 512), BF),
            pltpu.VMEM((512, 512), BF),
            pltpu.VMEM((2, 4, 32, 512), F32),
            pltpu.VMEM((2, 4, 32, 512), F32),
            pltpu.VMEM((2, 4, 32, 512), F32),
            pltpu.VMEM((2, 2, 4, 16, 512), F32),
            pltpu.VMEM((256, 128), F32),
            pltpu.VMEM((32, 8, 128), F32),
            pltpu.VMEM((32, 256, 512), BF),
            pltpu.VMEM((32, 128, 512), BF),
            pltpu.VMEM((512, 256), F32),
            pltpu.VMEM((2, 256, 128), F32),
            pltpu.VMEM((32 * HS, 128), F32),
            pltpu.VMEM((64 * FS, 128), F32),
            pltpu.VMEM((4, 256, 128), F32),
            pltpu.VMEM((2, 256, 128), F32),
            pltpu.VMEM((2, 32, 1024), F32),
        ] + sems + [pltpu.SemaphoreType.DMA, pltpu.SemaphoreType.DMA],
        compiler_params=pltpu.CompilerParams(
            vmem_limit_bytes=56 << 20, collective_id=0, has_side_effects=True
        ),
        name="panel",
    )(rot, pot, coef, idx, counts, *consts)


def per_device(coefficients, rotation, potential, index_map, counts):
    coef = coefficients.reshape(256, 2, 4, 128).transpose(0, 2, 1, 3).reshape(2048, 128)
    return run(
        rotation.transpose(0, 2, 1), potential, coef, index_map.reshape(128, 128), counts
    )


def solution(mesh):
    torus = Mesh(mesh.devices.reshape(4, 4, 2, 4, 2), GA + BAND)
    return jax.shard_map(
        per_device,
        mesh=torus,
        in_specs=(P(BAND, None, GA), P(None, BAND, GA), P(None, GA), P(), P()),
        out_specs=P(BAND + GA, None, None, None),
        check_vma=False,
    )
```

```python
import math

import jax
import jax.numpy as jnp
import numpy as np
from jax import lax
from jax.experimental import pallas as pl
from jax.experimental.pallas import tpu as pltpu
from jax.sharding import Mesh
from jax.sharding import PartitionSpec as P

F32 = jnp.float32
BF = jnp.bfloat16
MESH = pl.DeviceIdType.MESH
GA = ("ga_0", "ga_1", "ga_2")
BAND = ("band_0", "band_1")
HS = 72
FS = 40


def split_np(a):
    a = np.asarray(a, np.float32)
    hi = a.astype(BF)
    lo = (a - hi.astype(np.float32)).astype(BF)
    return hi, lo


def stack3(a):
    hi, lo = split_np(a)
    return np.concatenate([hi, hi, lo], axis=1)


def tables():
    n = np.arange(32) - 16
    r = np.arange(64)
    ang = 2.0 * math.pi * ((r[:, None] * n[None, :]) % 64) / 64.0
    cos, sin = np.cos(ang), np.sin(ang)
    perm = np.array([(k % 8) * 4 + k // 8 for k in range(32)])
    wz = np.zeros((2, 4, 32, 4, 2, 64))
    for q in range(4):
        wz[0, q, :, q, 0, :] = cos.T / 64
        wz[1, q, :, q, 0, :] = -sin.T / 64
        wz[0, q, :, q, 1, :] = sin.T / 64
        wz[1, q, :, q, 1, :] = cos.T / 64
    wz_h, wz_l = split_np(wz.reshape(256, 512))
    ty = stack3(np.concatenate([cos[:, perm], sin[:, perm]], axis=1) / 64)
    tx = stack3(np.concatenate([cos, sin], axis=1) / 64)
    fx = stack3(np.concatenate([cos.T, sin.T], axis=0))
    fy = stack3(np.concatenate([cos.T[perm], sin.T[perm]], axis=0))
    wf = np.zeros((4, 2, 64, 2, 4, 32))
    for q in range(4):
        wf[q, 0, :, 0, q, :] = cos
        wf[q, 1, :, 0, q, :] = sin
        wf[q, 1, :, 1, q, :] = cos
        wf[q, 0, :, 1, q, :] = -sin
    wf_h, wf_l = split_np(wf.reshape(512, 256))
    return [wz_h, wz_l, ty, tx, fx, fy, wf_h, wf_l]


def split(a):
    hi = a.astype(BF)
    return hi, (a - hi.astype(F32)).astype(BF)


def dot(a, b):
    return jnp.dot(a, b, preferred_element_type=F32)


def kernel(
    rot_in, pot_in, coef_in, idx_in, counts_in,
    wz_h_in, wz_l_in, ty_in, tx_in, fx_in, fy_in, wf_h_in, wf_l_in,
    out,
    rot, pot, coef, idx, counts, wz_h, wz_l, ty, tx, fx, fy, wf_h, wf_l,
    rg, vg, ch, cl, sb, sr, pb, rz, ab, vals, cols, rows, acc, ek, h, f, gz, o, res,
    l_sem, r_send, r_recv, v_send, v_recv, s_send, s_recv, z_send, z_recv,
    a_send, a_recv, w_send, w_recv,
):
    y, x, zh = lax.axis_index("ga_0"), lax.axis_index("ga_1"), lax.axis_index("ga_2")
    zl, core = lax.axis_index("band_0"), lax.axis_index("band_1")
    g = y * 8 + x * 2 + zh
    far = y * 8 + x * 2 + (1 - zh)
    half = pl.multiple_of(core * 32, 32)
    other = {"ga_2": 1 - zh}
    sibling = {"band_1": 1 - core}

    local = [
        pltpu.make_async_copy(a, b, l_sem.at[n])
        for n, (a, b) in enumerate([
            (rot_in.at[:, :, 0:128], rot.at[0]), (coef_in, coef), (pot_in, pot), (idx_in, idx),
            (counts_in, counts), (wz_h_in, wz_h), (wz_l_in, wz_l), (ty_in, ty),
            (tx_in, tx), (fx_in, fx), (fy_in, fy), (wf_h_in, wf_h), (wf_l_in, wf_l),
            (rot_in.at[:, :, 128:256], rot.at[1]),
        ])
    ]
    local[0].start()
    local[13].start()

    def mate(i):
        a, b = i // 4, i % 4
        yy = (y + (a ^ (a >> 1))) % 4
        xx = (x + (b ^ (b >> 1))) % 4
        return yy * 4 + xx, {"ga_0": yy, "ga_1": xx}

    barrier = pltpu.get_barrier_semaphore()

    def greet(i, _):
        pl.semaphore_signal(barrier, inc=1, device_id=mate(16 - i)[1], device_id_type=MESH)
        return 0

    def hop(i, _):
        p = (zl * 2 + core + i) % 8
        to = {"band_0": p // 2, "band_1": p % 2}
        pl.semaphore_signal(barrier, inc=1, device_id=to, device_id_type=MESH)
        return 0

    pl.semaphore_signal(barrier, inc=1, device_id=other, device_id_type=MESH)
    lax.fori_loop(1, 16, greet, 0)
    lax.fori_loop(1, 8, hop, 0)

    for n in range(1, 13):
        local[n].start()
    local[0].wait()
    local[13].wait()
    for t in range(2):
        for s in range(2):
            for r in range(2):
                rg[g, s, r * 4 : r * 4 + 4, t * 128 : t * 128 + 128] = rot[
                    t, r, pl.ds(s, 4, stride=2), :
                ]
    local[2].wait()
    vg[g, pl.ds(half, 32), :] = pot[pl.ds(half, 32), :]
    pl.semaphore_wait(barrier, 23)

    def send(src, dst, send_sem, recv_sem, to):
        return pltpu.make_async_remote_copy(
            src_ref=src, dst_ref=dst, send_sem=send_sem, recv_sem=recv_sem,
            device_id=to, device_id_type=MESH,
        )

    def rot_copy(block, i, to):
        return send(rg.at[block], rg.at[block], r_send.at[i], r_recv.at[block], to)

    def pot_copy(block, i, to):
        piece = vg.at[block, pl.ds(half, 32)]
        return send(piece, piece, v_send.at[i], v_recv.at[block], to)

    def each(lo, copy, hi=16):
        def step(i, _):
            copy(i).start()
            return 0

        lax.fori_loop(lo, hi, step, 0)

    rot_copy(g, 0, other).start()
    each(1, lambda i: rot_copy(g, i, mate(i)[1]))
    pot_copy(g, 0, other).start()

    local[1].wait()
    for c in range(2):
        for t in range(4):
            hi, lo = split(coef[pl.ds(t * 2 + c, 256, stride=8), :])
            ch[c * 256 : c * 256 + 256, t * 128 : t * 128 + 128] = hi
            cl[c * 256 : c * 256 + 256, t * 128 : t * 128 + 128] = lo

    local[3].wait()
    local[4].wait()
    rows128 = lax.broadcasted_iota(jnp.int32, (128, 512), 0)
    rows256 = lax.broadcasted_iota(jnp.int32, (256, 512), 0)
    slot = lax.broadcasted_iota(jnp.int32, (1, 512), 1)

    def one_hot(k, _):
        cell = jnp.concatenate([idx[pl.ds(k * 4 + t, 1), :] for t in range(4)], axis=1)
        wx = ((cell >> 12) + 16) & 63
        wy = ((cell >> 6) + 16) & 63
        wz = (cell + 16) & 63
        at_lane = (wx & 7) * 32 + wz
        at_row = (wx >> 3) * 32 + (wy & 3) * 8 + ((wy >> 2) & 7)
        at_row = jnp.where(slot < counts[k], at_row, -1)
        cols[k] = jnp.where(rows256 == at_lane, 1.0, 0.0).astype(BF)
        rows[k] = jnp.where(rows128 == at_row, 1.0, 0.0).astype(BF)
        return 0

    acc[...] = jnp.zeros_like(acc)
    sub = lax.broadcasted_iota(jnp.int32, (8, 256), 0)
    flip = jnp.where(sub < 4, -1.0, 1.0).astype(F32)

    def row_of(n):
        return (y + (n ^ (n >> 1))) % 4

    def plane_of(q):
        return zh if q == 0 else 1 - zh

    def pair_copy(q, d):
        return send(sb.at[q, d], sr.at[q, d], s_send.at[q * 4 + d], s_recv.at[q * 4 + d], sibling)

    def chip_copy(q, d, away, src):
        to = {"band_0": d, **sibling}
        if away:
            to["ga_2"] = 1 - zh
        return send(
            pb.at[q, d, pl.ds(away * 16, 16)], rz.at[q, away, src],
            z_send.at[q * 8 + d * 2 + away], z_recv.at[q * 8 + src * 2 + away], to,
        )

    def mix(q, n):
        d = row_of(n)

        def rot_wait(i, _):
            p, to = mate(i)
            rot_copy(p * 2 + plane_of(q), 0, to).wait_recv()
            return 0

        lax.fori_loop(max(1, n * 4), n * 4 + 4, rot_wait, 0)
        left, right = [], []
        for parity in (1 - core, core):
            for t in (zh, 1 - zh):
                for xb in range(2):
                    block = rg[d * 8 + (parity * 2 + xb) * 2 + plane_of(q), t]
                    left.append(block)
                    right.append(flip * pltpu.roll(block, 4, 0))
        lh, ll = split(jnp.concatenate([jnp.concatenate(left, 0), jnp.concatenate(right, 0)], 1))
        high = dot(jnp.concatenate([lh, ll], axis=0), ch[...])
        both = high[0:64] + high[64:128] + dot(lh, cl[...])
        sb[q, d] = both[0:32]
        pb[q, d] = both[32:64]
        pair_copy(q, d).start()

    def settle(q, n):
        d = row_of(n)
        pair_copy(q, d).wait_recv()
        pb[q, d] = pb[q, d] + sr[q, d]
        chip_copy(q, d, 0, zl).start()
        chip_copy(q, d, 1, zl).start()

    def band_copy(q, i):
        away, xb, xx = 1 - i // 8, (i // 4) % 2, (x + 3 - i % 4) % 4
        source = plane_of(away)
        yy = xb * 2 + plane_of(q ^ away)
        slot16 = yy * 4 + xx
        src = ab.at[pl.ds(pl.multiple_of(away * 128 + slot16 * 8, 8), 8)]
        block = (y * 4 + x) * 2 + source
        to = {"ga_0": yy, "ga_1": xx, **sibling}
        return send(
            src, vals.at[block], a_send.at[away * 16 + slot16], a_recv.at[block], to
        )

    def finish(q):
        for away in (1, 0):
            total = None
            for src in range(4):
                chip_copy(q, zl, away, src).wait_recv()
                part = rz[q, away, src]
                total = part if total is None else total + part
            for xb in range(2):
                for c in range(2):
                    for t in range(4):
                        start = away * 128 + (xb * 2 + plane_of(q ^ away)) * 32 + c * 4 + t
                        at = xb * 8 + c * 4
                        ab[pl.ds(start, 4, stride=8), :] = total[at : at + 4, t * 128 : t * 128 + 128]
            for i in range(8):
                band_copy(q, i + 8 * (1 - away)).start()

    lax.fori_loop(0, 32, one_hot, 0)
    mix(0, 0)
    rot_copy(far, 16, other).wait_recv()
    each(1, lambda i: rot_copy(far, 16 + i, mate(i)[1]))
    mix(0, 1)
    settle(0, 0)
    mix(0, 2)
    settle(0, 1)
    mix(0, 3)
    settle(0, 2)
    mix(1, 0)
    settle(0, 3)
    mix(1, 1)
    settle(1, 0)
    each(1, lambda i: pot_copy(g, i, mate(i)[1]))
    mix(1, 2)
    settle(1, 1)
    mix(1, 3)
    settle(1, 2)
    settle(1, 3)
    pot_copy(far, 16, other).wait_recv()
    each(1, lambda i: pot_copy(far, 16 + i, mate(i)[1]))
    finish(0)
    def pot_wait(i, _):
        p, to = mate(i)
        pot_copy(p * 2, 0, to).wait_recv()
        pot_copy(p * 2 + 1, 0, to).wait_recv()
        return 0

    lax.fori_loop(1, 16, pot_wait, 0)
    side = vg.at[:, pl.ds(half, 32)]
    swap = send(side, side, w_send, w_recv, sibling)
    swap.start()
    finish(1)
    def place(i, plane):
        left, right = [], []
        for b in range(4):
            k = mate(i * 4 + b)[0] * 2 + plane
            send(ab.at[pl.ds(0, 8)], vals.at[k], a_send.at[0], a_recv.at[k], sibling).wait_recv()

        for b in range(4):
            k = mate(i * 4 + b)[0] * 2 + plane
            hit = rows[k]
            parts = []
            for c in range(2):
                v = jnp.concatenate([vals[k, pl.ds(c * 4 + t, 1), :] for t in range(4)], axis=1)
                high = v.astype(BF).astype(F32)
                for part in (high, v - high):
                    wide = jnp.broadcast_to(part, (16, 512)).astype(BF)
                    parts.append(hit * jnp.concatenate([wide] * 8, axis=0))
            left.append(jnp.concatenate(parts, axis=0))
            right.append(cols[k])
        return lax.dot_general(
            jnp.concatenate(left, axis=1), jnp.concatenate(right, axis=1),
            (((1,), (1,)), ((), ())), preferred_element_type=F32,
        )

    soon = y % 2
    def place_step(i, _):
        acc[...] += place(i % 4, jnp.where(i < 4, soon, 1 - soon))
        return 0

    lax.fori_loop(0, 8, place_step, 0)

    for copy in local[5:13]:
        copy.wait()
    lane = lax.broadcasted_iota(jnp.int32, (1, 128), 1)
    turn = jnp.where(lane < 64, -1.0, 1.0).astype(F32)
    re = acc[0:128, :] + acc[128:256, :]
    im = acc[256:384, :] + acc[384:512, :]
    both = jnp.concatenate([re, im], axis=1)
    d = jnp.concatenate(
        [
            jnp.concatenate([v[:, t * 128 : t * 128 + 128] for v in (re, im)], axis=1)
            for t in range(2)
        ],
        axis=0,
    )
    dh, dl = split(d)
    e = dot(dh, wz_h[...]) + dot(dl, wz_h[...]) + dot(dh, wz_l[...])

    lane8 = lax.broadcasted_iota(jnp.int32, (8, 128), 1)
    high = lax.broadcasted_iota(jnp.int32, (8, 128), 0)
    ny = (high * 4 + (lane8 >> 5) - 16).astype(F32)
    nz = ((lane8 & 31) - 16).astype(F32)
    kyz = (8.0 / 4096.0) * (ny * ny + nz * nz)
    quarter = lax.broadcasted_iota(jnp.int32, (1, 128), 1) >> 5
    lines = [
        jnp.concatenate(
            [
                both[xh * 32 + j * 8 : xh * 32 + j * 8 + 8, ct * 128 : ct * 128 + 128]
                for ct in range(4)
                for xh in range(4)
            ],
            axis=0,
        )
        for j in range(4)
    ]
    for q in range(4):
        turned = [
            lines[j] if j == q else pltpu.roll(lines[j], ((j - q) * 32) % 128, 1) for j in range(4)
        ]
        mixed = jnp.where(
            quarter < 2,
            jnp.where(quarter == 0, turned[0], turned[1]),
            jnp.where(quarter == 2, turned[2], turned[3]),
        )
        for ct in range(4):
            for xh in range(4):
                i = xh * 8 + (ct % 2) * 4 + q
                kin = kyz + (8.0 / 4096.0) * (i - 16) ** 2
                at = (ct * 4 + xh) * 8
                ek[ct // 2, i * 8 : i * 8 + 8, :] = kin * mixed[at : at + 8, :]

    def column(i):
        xh, t, q = i // 8, (i // 4) % 2, i % 4
        at = t * 128 + xh * 32
        tile = e[at : at + 32, q * 128 : q * 128 + 128]
        return jnp.concatenate([tile, turn * pltpu.roll(tile, 64, 1)], axis=0)

    for i in range(0, 32, 2):
        dh, dl = split(jnp.concatenate([column(i), column(i + 1)], axis=1))
        d = dot(ty[...], jnp.concatenate([dh, dl, dh], axis=0))
        h[i * HS : i * HS + 64, :] = d[:, 0:128]
        h[(i + 1) * HS : (i + 1) * HS + 64, :] = d[:, 128:256]

    swap.wait()

    def plane(i, _):
        both = []
        for q in range(2):
            tile = h[pl.ds(i * 2 + q, 32, stride=HS), :]
            both.append(jnp.concatenate([tile, turn * pltpu.roll(tile, 64, 1)], axis=0))
        dh, dl = split(jnp.concatenate(both, axis=1))
        real = dot(tx[...], jnp.concatenate([dh, dl, dh], axis=0))
        v = vg[i]
        vr = pltpu.roll(v, 64, 1)
        low = lane < 64
        vv = jnp.concatenate([jnp.where(low, v, vr), jnp.where(low, vr, v)], axis=1)
        dh, dl = split(real * vv)
        pq = dot(fx[...], jnp.concatenate([dh, dl, dh], axis=0))
        for q in range(2):
            pp = pq[0:32, q * 128 : q * 128 + 128]
            qq = pq[32:64, q * 128 : q * 128 + 128]
            start = pl.multiple_of((i * 2 + q) * FS, 8)
            f[pl.ds(start, 32), :] = pp - turn * pltpu.roll(qq, 64, 1)
        return 0

    lax.fori_loop(0, 32, plane, 0, unroll=32)

    def line(i, _):
        d = jnp.concatenate([f[pl.ds(i * 2 + q, 64, stride=FS), :] for q in range(2)], axis=1)
        dh, dl = split(d)
        pq = dot(fy[...], jnp.concatenate([dh, dl, dh], axis=0))
        for q in range(2):
            pp = pq[0:32, q * 128 : q * 128 + 128]
            qq = pq[32:64, q * 128 : q * 128 + 128]
            yy = pp - turn * pltpu.roll(qq, 64, 1)
            start = pl.multiple_of((i * 2 + q) * 8, 8)
            for j in range(4):
                gz[j, pl.ds(start, 8), :] = yy[j * 8 : j * 8 + 8, :]
        return 0

    lax.fori_loop(0, 16, line, 0, unroll=16)

    dh, dl = split(jnp.concatenate([gz[j] for j in range(4)], axis=1))
    z = dot(dh, wf_h[...]) + dot(dl, wf_h[...]) + dot(dh, wf_l[...])
    def result(c):
        return pltpu.make_async_copy(res.at[c], out.at[0, c], l_sem.at[c])

    for c in range(2):
        o[c] = z[:, c * 128 : c * 128 + 128] + ek[c]
        for b in range(8):
            res[c, :, b * 128 : b * 128 + 128] = o[c, pl.ds(b, 32, stride=8), :]
        result(c).start()

    rot_copy(g, 0, other).wait_send()
    pot_copy(g, 0, other).wait_send()

    def sent(i, _):
        to = mate(i)[1]
        rot_copy(g, i, to).wait_send()
        rot_copy(far, 16 + i, to).wait_send()
        pot_copy(g, i, to).wait_send()
        pot_copy(far, 16 + i, to).wait_send()
        return 0

    lax.fori_loop(1, 16, sent, 0)
    for q in range(2):
        for d in range(4):
            pair_copy(q, d).wait_send()
            chip_copy(q, d, 1, 0).wait_send()
            chip_copy(q, d, 0, 0).wait_send()
        for i in range(16):
            band_copy(q, i).wait_send()
    for c in range(2):
        result(c).wait()


def run(rot, pot, coef, idx, counts):
    consts = [jnp.asarray(c) for c in tables()]
    hbm = pl.BlockSpec(memory_space=pltpu.HBM)
    sems = [pltpu.SemaphoreType.DMA((n,)) for n in (14, 32, 32, 32, 32, 8, 8, 16, 16, 32, 32)]
    return pl.pallas_call(
        kernel,
        out_shape=jax.ShapeDtypeStruct((1, 2, 32, 1024), F32),
        in_specs=[hbm] * 13,
        out_specs=hbm,
        scratch_shapes=[
            pltpu.VMEM((2, 2, 8, 128), F32),
            pltpu.VMEM((64, 128), F32),
            pltpu.VMEM((2048, 128), F32),
            pltpu.VMEM((128, 128), jnp.int32),
            pltpu.SMEM((32,), jnp.int32),
        ] + [pltpu.VMEM(c.shape, c.dtype) for c in consts] + [
            pltpu.VMEM((32, 2, 8, 256), F32),
            pltpu.VMEM((32, 64, 128), F32),
            pltpu.VMEM((512, 512), BF),
            pltpu.VMEM((512, 512), BF),
            pltpu.VMEM((2, 4, 32, 512), F32),
            pltpu.VMEM((2, 4, 32, 512), F32),
            pltpu.VMEM((2, 4, 32, 512), F32),
            pltpu.VMEM((2, 2, 4, 16, 512), F32),
            pltpu.VMEM((256, 128), F32),
            pltpu.VMEM((32, 8, 128), F32),
            pltpu.VMEM((32, 256, 512), BF),
            pltpu.VMEM((32, 128, 512), BF),
            pltpu.VMEM((512, 256), F32),
            pltpu.VMEM((2, 256, 128), F32),
            pltpu.VMEM((32 * HS, 128), F32),
            pltpu.VMEM((64 * FS, 128), F32),
            pltpu.VMEM((4, 256, 128), F32),
            pltpu.VMEM((2, 256, 128), F32),
            pltpu.VMEM((2, 32, 1024), F32),
        ] + sems + [pltpu.SemaphoreType.DMA, pltpu.SemaphoreType.DMA],
        compiler_params=pltpu.CompilerParams(
            vmem_limit_bytes=56 << 20, collective_id=0, has_side_effects=True
        ),
        name="panel",
    )(rot, pot, coef, idx, counts, *consts)


def per_device(coefficients, rotation, potential, index_map, counts):
    coef = coefficients.reshape(256, 2, 4, 128).transpose(0, 2, 1, 3).reshape(2048, 128)
    return run(
        rotation.transpose(0, 2, 1), potential, coef, index_map.reshape(128, 128), counts
    )


def solution(mesh):
    torus = Mesh(mesh.devices.reshape(4, 4, 2, 4, 2), GA + BAND)
    return jax.shard_map(
        per_device,
        mesh=torus,
        in_specs=(P(BAND, None, GA), P(None, BAND, GA), P(None, GA), P(), P()),
        out_specs=P(BAND + GA, None, None, None),
        check_vma=False,
    )
```
